32 devices in a mesh: tp: 4 (over z), dp: 8 (over y, x, core).
Axes of the slice: x: 2, y: 2, z: 4, core: 2. Of those that a mesh axis runs over, the one named last changes fastest.
Arguments:
- design: float32 [49152, 2560], P('dp', 'tp')
- target: float32 [49152], P('dp')
- ridge: float32 [], replicated
Outputs:
- output 1: float32 [2560], replicated
- output 2: float32 [49152], P('dp')
All inputs are finite; a program needn't handle non-finite values.
Results may differ from the reference program's by a relative error of at most 0.001.
Values sent between devices are 32-bit elements.
A program may use at most 1 GiB of HBM per device.

```python
import jax
import jax.numpy as jnp
from jax import lax

FEATURES = 2560
ROWS_DEV = 6144
GROUPS = 8
LOW_RANK = 128

TOTAL_ROWS = ROWS_DEV * GROUPS
HIGHEST = lax.Precision.HIGHEST
CONTRACT_ROWS = (((0,), (0,)), ((), ()))


def setup_inputs(seed: int = 0) -> dict:
    keys = jax.random.split(jax.random.key(seed), 9)
    col_scale = jnp.exp(jax.random.uniform(keys[0], (FEATURES,), jnp.float32, -3.0, 0.0))
    base = jax.random.normal(keys[1], (TOTAL_ROWS, FEATURES), jnp.float32)
    factors = jax.random.normal(keys[2], (TOTAL_ROWS, LOW_RANK), jnp.float32)
    mixing = jax.random.normal(keys[3], (FEATURES, LOW_RANK), jnp.float32) * (0.5 * LOW_RANK ** -0.5)
    shard_gain = jnp.exp(jax.random.uniform(keys[4], (GROUPS, 1), jnp.float32, -1.0, 1.0))
    row_jitter = jnp.exp(jax.random.uniform(keys[5], (GROUPS, ROWS_DEV), jnp.float32, -0.25, 0.25))
    row_gain = (shard_gain * row_jitter).reshape(TOTAL_ROWS, 1)
    mixed = jnp.dot(factors, mixing.T, precision=HIGHEST)
    design = (base * col_scale + mixed) * (row_gain * FEATURES ** -0.5)
    x_true = jax.random.normal(keys[6], (FEATURES,), jnp.float32)
    noise = 0.3 * jax.random.normal(keys[7], (TOTAL_ROWS,), jnp.float32) * row_gain[:, 0]
    target = jnp.dot(design, x_true, precision=HIGHEST) + noise
    diag_mean = jnp.sum(design * design) / FEATURES
    ridge = diag_mean * jax.random.uniform(keys[8], (), jnp.float32, 0.01, 0.04)
    return {'design': design, 'target': target, 'ridge': ridge}


def reference(design, target, ridge):
    gram_mat = lax.dot_general(design, design, CONTRACT_ROWS, precision=HIGHEST, preferred_element_type=jnp.float32)
    moment_vec = lax.dot_general(design, target, CONTRACT_ROWS, precision=HIGHEST, preferred_element_type=jnp.float32)
    chol_low = jnp.linalg.cholesky(gram_mat + ridge * jnp.eye(FEATURES, dtype=jnp.float32))
    half_solve = lax.linalg.triangular_solve(chol_low, moment_vec[:, None], left_side=True, lower=True)
    coeffs = lax.linalg.triangular_solve(chol_low, half_solve, left_side=True, lower=True, transpose_a=True)[:, 0]
    residual = target - jnp.dot(design, coeffs, precision=HIGHEST, preferred_element_type=jnp.float32)
    return coeffs, residual
```

```python
import functools

import jax
import jax.numpy as jnp
from jax import lax
from jax.experimental import pallas as pl
from jax.experimental.pallas import tpu as pltpu
from jax.sharding import PartitionSpec as P


LANES = 128
SUB = 8
BLK = 128
NB = 512
F32 = jnp.float32
BF16 = jnp.bfloat16


def split3(x):
    hi = x.astype(BF16)
    rest = x - hi.astype(F32)
    mid = rest.astype(BF16)
    low = (rest - mid.astype(F32)).astype(BF16)
    return hi, mid, low


def lhs_cat(x):
    hi, mid, low = split3(x)
    return jnp.concatenate([hi, mid, hi, low, mid, hi], axis=1)


def rhs_cat(x):
    hi, mid, low = split3(x)
    return jnp.concatenate([mid, hi, low, hi, mid, hi], axis=0)


def dot_cat(lhs, rhs):
    return lax.dot_general(lhs, rhs, (((1,), (0,)), ((), ())), preferred_element_type=F32)


def row_sums(parts, sub):
    for shift in (4, 2, 1):
        low = (sub & shift) == 0
        nxt = []
        for t in range(shift):
            a, b = parts[t], parts[t + shift]
            keep = jnp.where(low, a, b)
            move = jnp.where(low, b, a)
            nxt.append(keep + xor_roll(move, shift, sub))
        parts = nxt
    return parts[0]


def xor_roll(x, shift, sub):
    if shift == 4:
        return pltpu.roll(x, 4, 0)
    low = (sub & shift) == 0
    return jnp.where(low, pltpu.roll(x, SUB - shift, 0), pltpu.roll(x, shift, 0))


def bcast_lane(x, c):
    return jnp.broadcast_to(x[:, c:c + 1], (SUB, LANES))


def bcast_row(x, p):
    return jnp.broadcast_to(x[p:p + 1, :], (SUB, LANES))


def factor_block(load, sub, lane):
    octs = BLK // SUB
    a = [load(o) for o in range(octs)]
    e = [jnp.where(lane == sub + SUB * o, 1.0, 0.0).astype(F32) for o in range(octs)]
    out = [None] * octs
    for t in range(octs // 2):
        o0, o1 = 2 * t, 2 * t + 1
        c0 = 16 * t
        r0, r1, e0, e1 = a[o0], a[o1], e[o0], e[o1]
        b0 = [bcast_lane(r0, c0 + q) for q in range(16)]
        b1 = [bcast_lane(r1, c0 + q) for q in range(16)]
        d0 = jnp.ones((SUB, LANES), F32)
        d1 = jnp.ones((SUB, LANES), F32)
        for p in range(16):
            ps = p % 8
            first = p < 8
            piv = bcast_row(b0[p] if first else b1[p], ps)
            inv = 1.0 / piv
            if first:
                d0 = jnp.where(sub == ps, piv, d0)
                m0 = jnp.where(sub > ps, b0[p] * inv, 0.0)
                m1 = b1[p] * inv
            else:
                d1 = jnp.where(sub == ps, piv, d1)
                m1 = jnp.where(sub > ps, b1[p] * inv, 0.0)
            for q in range(p + 1, 16):
                row = bcast_row(b0[q] if first else b1[q], ps)
                if first and ps < 7:
                    b0[q] = b0[q] - m0 * row
                b1[q] = b1[q] - m1 * row
            rr, re = bcast_row(r0 if first else r1, ps), bcast_row(e0 if first else e1, ps)
            if first and ps < 7:
                r0 = r0 - m0 * rr
                e0 = e0 - m0 * re
            r1 = r1 - m1 * rr
            e1 = e1 - m1 * re
        s0, s1 = lax.rsqrt(d0), lax.rsqrt(d1)
        u0, u1, v0, v1 = r0 * s0, r1 * s1, e0 * s0, e1 * s1
        out[o0], out[o1] = v0, v1
        for o in range(2 * t + 2, octs):
            xs, ys = [], []
            for k in range(SUB):
                i = SUB * o + k
                g0, g1 = bcast_lane(u0, i), bcast_lane(u1, i)
                xs.append(g0 * u0 + g1 * u1)
                ys.append(g0 * v0 + g1 * v1)
            a[o] = a[o] - row_sums(xs, sub)
            e[o] = e[o] - row_sums(ys, sub)
    return out


def diag_kernel(lam_ref, s_ref, w_ref, work):
    n = s_ref.shape[0]
    steps = n // BLK
    sub = lax.broadcasted_iota(jnp.int32, (SUB, LANES), 0)
    lane = lax.broadcasted_iota(jnp.int32, (SUB, LANES), 1)
    row = lax.broadcasted_iota(jnp.int32, (n, n), 0)
    col = lax.broadcasted_iota(jnp.int32, (n, n), 1)
    work[:, :n] = s_ref[...] + jnp.where(row == col, lam_ref[0], 0.0)
    work[:, n:] = jnp.where(row == col, 1.0, 0.0)

    def step(k, carry):
        base = pl.multiple_of(k * BLK, BLK)
        win = pl.ds(pl.multiple_of(base + BLK, BLK), n)
        diag = pl.ds(base, BLK)

        def load(o):
            return work[pl.ds(pl.multiple_of(base + SUB * o, SUB), SUB), diag]

        inv = jnp.concatenate(factor_block(load, sub, lane), axis=0)
        panel = dot_cat(lhs_cat(inv), rhs_cat(work[diag, win]))
        work[diag, win] = panel
        right = rhs_cat(panel)
        for j in range(steps - 1):
            @pl.when(k == j)
            def _(j=j):
                rows = n - BLK * (j + 1)
                left = lhs_cat(panel[:, :rows].T)
                w = (pl.ds(BLK * (j + 1), rows), pl.ds(BLK * (j + 1), n))
                work[w] = work[w] - dot_cat(left, right)
        return carry

    lax.fori_loop(0, steps, step, 0)
    w_ref[...] = work[:, n:]


def diag_inverse(sdiag, lam):
    n = sdiag.shape[0]
    return pl.pallas_call(
        diag_kernel,
        out_shape=jax.ShapeDtypeStruct((n, n), F32),
        in_specs=[pl.BlockSpec(memory_space=pltpu.SMEM), pl.BlockSpec(memory_space=pltpu.VMEM)],
        out_specs=pl.BlockSpec(memory_space=pltpu.VMEM),
        scratch_shapes=[pltpu.VMEM((n, 2 * n), F32)],
        cost_estimate=pl.CostEstimate(flops=20_000_000_000, bytes_accessed=8 * n * n, transcendentals=0),
        name="diag_inverse",
    )(lam.reshape(1), sdiag)


def solve_kernel(n, h_ref, *refs):
    pairs = [(j, c) for c in range(n) for j in range(c)]
    u_refs = dict(zip(pairs, refs[:len(pairs)]))
    w_refs = refs[len(pairs):len(pairs) + n]
    x_ref = refs[len(pairs) + n]
    half = []
    for c in range(n):
        right = h_ref[c:c + 1, :]
        for j in range(c):
            right = right - jnp.sum(u_refs[j, c][...] * half[j], axis=0, keepdims=True)
        half.append(jnp.sum(w_refs[c][...] * right, axis=1, keepdims=True))
    for c in reversed(range(n)):
        left = half[c]
        for k in range(c + 1, n):
            left = left - jnp.sum(u_refs[c, k][...] * x_ref[k:k + 1, :], axis=1, keepdims=True)
        x_ref[c:c + 1, :] = jnp.sum(w_refs[c][...] * left, axis=0, keepdims=True)


def solve(moment, uppers, inverses):
    n = len(inverses)
    blocks = [uppers[j, c] for c in range(n) for j in range(c)]
    return pl.pallas_call(
        functools.partial(solve_kernel, n),
        out_shape=jax.ShapeDtypeStruct((n, NB), F32),
        in_specs=[pl.BlockSpec(memory_space=pltpu.VMEM)] * (1 + len(blocks) + n),
        out_specs=pl.BlockSpec(memory_space=pltpu.VMEM),
        compiler_params=pltpu.CompilerParams(vmem_limit_bytes=40 * 1024 * 1024),
        cost_estimate=pl.CostEstimate(flops=5_000_000_000, bytes_accessed=16_000_000, transcendentals=0),
        name="solve",
    )(moment, *blocks, *inverses)


HIGHEST = lax.Precision.HIGHEST
CONTRACT_ROWS = (((0,), (0,)), ((), ()))


def gram(left, right):
    return lax.dot_general(left, right, CONTRACT_ROWS, precision=HIGHEST, preferred_element_type=F32)


GROUPS = ((0, 1), (2,), (3,), (4,))


def swap(x, axis, ways, mask):
    return lax.ppermute(x, axis, [(i, i ^ mask) for i in range(ways)])


def pick(stack, i):
    return lax.dynamic_index_in_dim(stack, i, 0, keepdims=False)


def scatter_sum(x, me, ways, send):
    parts = x.reshape(ways, -1, x.shape[1])
    total = pick(parts, me)
    for m in range(1, ways):
        total = total + send(pick(parts, me ^ m), m)
    return total


def gather(x, me, ways, send):
    out = jnp.zeros((ways * x.shape[0], x.shape[1]), x.dtype)
    for m in range(ways):
        out = lax.dynamic_update_slice(out, send(x, m) if m else x, ((me ^ m) * x.shape[0], 0))
    return out


def sum_all(x, tp_ways, dp_ways):
    tp, dp = lax.axis_index('tp'), lax.axis_index('dp')
    core = (dp & 1, 2, lambda v, m: swap(v, 'dp', dp_ways, m))
    plane = (dp >> 1, dp_ways // 2, lambda v, m: swap(v, 'dp', dp_ways, 2 * m))
    column = (tp, tp_ways, lambda v, m: swap(v, 'tp', tp_ways, m))
    for level in (core, plane, column):
        x = scatter_sum(x, *level)
    part = x
    for level in (column, plane, core):
        x = gather(x, *level)
    return x, part


def solution(mesh):
    tp_ways, dp_ways = mesh.shape['tp'], mesh.shape['dp']

    def exchange(design_blk, tp, c, width, after):
        block = design_blk[:, width * c:width * (c + 1)].reshape(tp_ways, -1, width)
        if after is not None:
            block, _ = lax.optimization_barrier((block, after))
        got = [pick(block, tp)]
        for m in range(1, tp_ways):
            got.append(swap(pick(block, tp ^ m), 'tp', tp_ways, m))
        return got

    def local_fit(design_blk, target_blk, ridge):
        rows_dev, cols_dev = design_blk.shape
        sub_rows = rows_dev // tp_ways
        width = NB // tp_ways
        chunks = cols_dev // width
        tp = lax.axis_index('tp')
        target_part = lax.dynamic_slice_in_dim(target_blk, tp * sub_rows, sub_rows)
        target_pad = jnp.pad(target_part[:, None], ((0, 0), (0, SUB - 1)))

        got, cols, totals, uppers, inverses, moments = [], [], {}, {}, [], []
        for c in range(chunks):
            after = tuple(got[c - 2][1:]) if c >= 2 else None
            got.append(exchange(design_blk, tp, c, width, after))
            col = jnp.zeros((sub_rows, NB), F32)
            for m in range(tp_ways):
                col = lax.dynamic_update_slice(col, got[c][m], (0, (tp ^ m) * width))
            cols.append(col)
        part = None
        for group in GROUPS:
            parts = []
            for c in group:
                if part is not None:
                    cols[c], _ = lax.optimization_barrier((cols[c], part))
                blocks = [gram(cols[j], cols[c]) for j in range(c + 1)]
                moment = gram(target_pad, cols[c])[0]
                blocks[c] = lax.dynamic_update_slice(blocks[c], moment.reshape(2, NB // 2), (NB - 2, 0))
                parts += blocks
            total, part = sum_all(jnp.concatenate(parts, axis=0), tp_ways, dp_ways)
            row = 0
            for c in group:
                totals[c] = [total[row + NB * k:row + NB * (k + 1)] for k in range(c + 1)]
                row += NB * (c + 1)
            for c in group:
                moments.append(totals[c][c][-2:, :NB // 2].reshape(1, NB))
                for k in range(c + 1):
                    block = totals[c][k]
                    for j in range(k):
                        block = block - gram(uppers[j, k], uppers[j, c])
                    if k < c:
                        uppers[k, c] = jnp.dot(inverses[k], block, precision=HIGHEST, preferred_element_type=F32)
                    else:
                        inverses.append(diag_inverse(block, ridge))
        order = solve(jnp.concatenate(moments, axis=0), uppers, inverses)
        order = order.reshape(chunks, tp_ways, width)
        coeffs = order.transpose(1, 0, 2).reshape(-1)
        coeff_blk = lax.dynamic_index_in_dim(order, tp, 1, keepdims=False).reshape(-1)
        fitted = jnp.sum(design_blk * coeff_blk[None, :], axis=1)
        for k in range(tp_ways.bit_length() - 1):
            fitted = fitted + swap(fitted, 'tp', tp_ways, 1 << k)
        return coeffs, target_blk - fitted

    return jax.shard_map(local_fit, mesh=mesh, in_specs=(P('dp', 'tp'), P('dp'), P()), out_specs=(P(), P('dp')), check_vma=False)
```

```python
import functools

import jax
import jax.numpy as jnp
from jax import lax
from jax.experimental import pallas as pl
from jax.experimental.pallas import tpu as pltpu
from jax.sharding import PartitionSpec as P

LANES = 128
SUB = 8
BLK = 128
NB = 512
CHUNKS = 5
F32 = jnp.float32
BF16 = jnp.bfloat16


def split3(x):
    hi = x.astype(BF16)
    rest = x - hi.astype(F32)
    mid = rest.astype(BF16)
    low = (rest - mid.astype(F32)).astype(BF16)
    return hi, mid, low


def lhs_cat(x):
    hi, mid, low = split3(x)
    return jnp.concatenate([hi, mid, hi, low, mid, hi], axis=1)


def rhs_cat(x):
    hi, mid, low = split3(x)
    return jnp.concatenate([mid, hi, low, hi, mid, hi], axis=0)


def dot_cat(lhs, rhs):
    return lax.dot_general(lhs, rhs, (((1,), (0,)), ((), ())), preferred_element_type=F32)


def row_sums(parts, sub):
    for shift in (4, 2, 1):
        low = (sub & shift) == 0
        nxt = []
        for t in range(shift):
            a, b = parts[t], parts[t + shift]
            keep = jnp.where(low, a, b)
            move = jnp.where(low, b, a)
            nxt.append(keep + xor_roll(move, shift, sub))
        parts = nxt
    return parts[0]


def xor_roll(x, shift, sub):
    if shift == 4:
        return pltpu.roll(x, 4, 0)
    low = (sub & shift) == 0
    return jnp.where(low, pltpu.roll(x, SUB - shift, 0), pltpu.roll(x, shift, 0))


def bcast_lane(x, c):
    return jnp.broadcast_to(x[:, c:c + 1], (SUB, LANES))


def bcast_row(x, p):
    return jnp.broadcast_to(x[p:p + 1, :], (SUB, LANES))


def factor_block(load, sub, lane):
    octs = BLK // SUB
    a = [load(o) for o in range(octs)]
    e = [jnp.where(lane == sub + SUB * o, 1.0, 0.0).astype(F32) for o in range(octs)]
    out = [None] * octs
    for t in range(octs // 2):
        o0, o1 = 2 * t, 2 * t + 1
        c0 = 16 * t
        r0, r1, e0, e1 = a[o0], a[o1], e[o0], e[o1]
        b0 = [bcast_lane(r0, c0 + q) for q in range(16)]
        b1 = [bcast_lane(r1, c0 + q) for q in range(16)]
        d0 = jnp.ones((SUB, LANES), F32)
        d1 = jnp.ones((SUB, LANES), F32)
        for p in range(16):
            ps = p % 8
            first = p < 8
            piv = bcast_row(b0[p] if first else b1[p], ps)
            inv = 1.0 / piv
            if first:
                d0 = jnp.where(sub == ps, piv, d0)
                m0 = jnp.where(sub > ps, b0[p] * inv, 0.0)
                m1 = b1[p] * inv
            else:
                d1 = jnp.where(sub == ps, piv, d1)
                m1 = jnp.where(sub > ps, b1[p] * inv, 0.0)
            for q in range(p + 1, 16):
                row = bcast_row(b0[q] if first else b1[q], ps)
                if first and ps < 7:
                    b0[q] = b0[q] - m0 * row
                b1[q] = b1[q] - m1 * row
            rr, re = bcast_row(r0 if first else r1, ps), bcast_row(e0 if first else e1, ps)
            if first and ps < 7:
                r0 = r0 - m0 * rr
                e0 = e0 - m0 * re
            r1 = r1 - m1 * rr
            e1 = e1 - m1 * re
        s0, s1 = lax.rsqrt(d0), lax.rsqrt(d1)
        u0, u1, v0, v1 = r0 * s0, r1 * s1, e0 * s0, e1 * s1
        out[o0], out[o1] = v0, v1
        for o in range(2 * t + 2, octs):
            xs, ys = [], []
            for k in range(SUB):
                i = SUB * o + k
                g0, g1 = bcast_lane(u0, i), bcast_lane(u1, i)
                xs.append(g0 * u0 + g1 * u1)
                ys.append(g0 * v0 + g1 * v1)
            a[o] = a[o] - row_sums(xs, sub)
            e[o] = e[o] - row_sums(ys, sub)
    return out


def diag_kernel(lam_ref, s_ref, w_ref, work):
    n = s_ref.shape[0]
    steps = n // BLK
    sub = lax.broadcasted_iota(jnp.int32, (SUB, LANES), 0)
    lane = lax.broadcasted_iota(jnp.int32, (SUB, LANES), 1)
    row = lax.broadcasted_iota(jnp.int32, (n, n), 0)
    col = lax.broadcasted_iota(jnp.int32, (n, n), 1)
    work[:, :n] = s_ref[...] + jnp.where(row == col, lam_ref[0], 0.0)
    work[:, n:] = jnp.where(row == col, 1.0, 0.0)

    def step(k, carry):
        base = pl.multiple_of(k * BLK, BLK)
        win = pl.ds(pl.multiple_of(base + BLK, BLK), n)
        diag = pl.ds(base, BLK)

        def load(o):
            return work[pl.ds(pl.multiple_of(base + SUB * o, SUB), SUB), diag]

        inv = jnp.concatenate(factor_block(load, sub, lane), axis=0)
        panel = dot_cat(lhs_cat(inv), rhs_cat(work[diag, win]))
        work[diag, win] = panel
        right = rhs_cat(panel)
        for j in range(steps - 1):
            @pl.when(k == j)
            def _(j=j):
                rows = n - BLK * (j + 1)
                left = lhs_cat(panel[:, :rows].T)
                w = (pl.ds(BLK * (j + 1), rows), pl.ds(BLK * (j + 1), n))
                work[w] = work[w] - dot_cat(left, right)
        return carry

    lax.fori_loop(0, steps, step, 0)
    w_ref[...] = work[:, n:]


def diag_inverse(sdiag, lam):
    n = sdiag.shape[0]
    return pl.pallas_call(
        diag_kernel,
        out_shape=jax.ShapeDtypeStruct((n, n), F32),
        in_specs=[pl.BlockSpec(memory_space=pltpu.SMEM), pl.BlockSpec(memory_space=pltpu.VMEM)],
        out_specs=pl.BlockSpec(memory_space=pltpu.VMEM),
        scratch_shapes=[pltpu.VMEM((n, 2 * n), F32)],
        cost_estimate=pl.CostEstimate(flops=20_000_000_000, bytes_accessed=8 * n * n, transcendentals=0),
        name="diag_inverse",
    )(lam.reshape(1), sdiag)


def solve_kernel(n, h_ref, *refs):
    pairs = [(j, c) for c in range(n) for j in range(c)]
    u_refs = dict(zip(pairs, refs[:len(pairs)]))
    w_refs = refs[len(pairs):len(pairs) + n]
    x_ref = refs[len(pairs) + n]
    nb = w_refs[0].shape[0]
    half = []
    for c in range(n):
        right = h_ref[c:c + 1, :]
        for j in range(c):
            right = right - jnp.sum(u_refs[j, c][...] * half[j], axis=0, keepdims=True)
        half.append(jnp.sum(w_refs[c][...] * right, axis=1, keepdims=True))
    for c in reversed(range(n)):
        left = half[c]
        for k in range(c + 1, n):
            left = left - jnp.sum(u_refs[c, k][...] * x_ref[k:k + 1, :], axis=1, keepdims=True)
        x_ref[c:c + 1, :] = jnp.sum(w_refs[c][...] * left, axis=0, keepdims=True)


def solve(moment, uppers, inverses):
    n = len(inverses)
    blocks = [uppers[j, c] for c in range(n) for j in range(c)]
    return pl.pallas_call(
        functools.partial(solve_kernel, n),
        out_shape=jax.ShapeDtypeStruct((n, NB), F32),
        in_specs=[pl.BlockSpec(memory_space=pltpu.VMEM)] * (1 + len(blocks) + n),
        out_specs=pl.BlockSpec(memory_space=pltpu.VMEM),
        compiler_params=pltpu.CompilerParams(vmem_limit_bytes=40 * 1024 * 1024),
        cost_estimate=pl.CostEstimate(flops=5_000_000_000, bytes_accessed=16_000_000, transcendentals=0),
        name="solve",
    )(moment, *blocks, *inverses)


HIGHEST = lax.Precision.HIGHEST
CONTRACT_ROWS = (((0,), (0,)), ((), ()))


def gram(left, right):
    return lax.dot_general(left, right, CONTRACT_ROWS, precision=HIGHEST, preferred_element_type=F32)


MESH = pl.DeviceIdType.MESH
PIECES = 3
AHEAD = 2
SUMMED = ((0, 3), (3, 3), (6, 4))
READY = (5, 8, 11)


def ladder(tp_ways, dp_ways):
    return (("dp", 2, 1), ("dp", dp_ways // 2, 2), ("tp", tp_ways, 1))


def place(level):
    axis, ways, dist = level
    return lax.rem(lax.axis_index(axis) // dist, ways)


def member(level, m):
    axis, ways, dist = level
    return {axis: lax.axis_index(axis) ^ (m * dist)}


def sweep_kernel(levels, a_ref, b_ref, p_ref, x_ref, right, moment, got0, got1, got2, swap_send, swap_recv, own_sem, send_sem, recv_sem, free_sem):
    ways = levels[2][1]
    sub_rows = a_ref.shape[0] // ways
    width = a_ref.shape[1] // CHUNKS
    piece = sub_rows // PIECES
    steps = CHUNKS * PIECES
    z = lax.axis_index("tp")
    got = (got0, got1, got2)

    barrier = pltpu.get_barrier_semaphore()
    count = 0
    for level in levels:
        for m in range(1, level[1]):
            pl.semaphore_signal(barrier, inc=1, device_id=member(level, m), device_id_type=MESH)
            count += 1
    pl.semaphore_wait(barrier, count)

    def own(c):
        return pltpu.make_async_copy(
            a_ref.at[pl.ds(z * sub_rows, sub_rows), pl.ds(width * c, width)], x_ref.at[c, z], own_sem.at[c])

    def travel(p, m):
        c, r = p // PIECES, lax.rem(p, PIECES)
        rows = pl.ds(pl.multiple_of((z ^ m) * sub_rows + r * piece, SUB), piece)
        cols = pl.ds(pl.multiple_of(c * width, LANES), width)
        return pltpu.make_async_remote_copy(
            src_ref=a_ref.at[rows, cols],
            dst_ref=x_ref.at[c, z, pl.ds(pl.multiple_of(r * piece, SUB), piece)],
            send_sem=swap_send.at[p, m - 1],
            recv_sem=swap_recv.at[p, m - 1],
            device_id=member(levels[2], m),
            device_id_type=MESH,
        )

    def load(c, r):
        rows = pl.ds(pl.multiple_of(r * piece, SUB), piece)
        return jnp.concatenate([x_ref[c, t, rows, :] for t in range(ways)], axis=1)

    def span(g, depth):
        first, n = SUMMED[g]
        start, rows = first * NB, n * NB
        for level in levels[:depth]:
            rows //= level[1]
            start = start + place(level) * rows
        return start, rows

    def part(g, depth, m):
        start, _ = span(g, depth)
        rows = span(g, depth + 1)[1]
        return pl.ds(pl.multiple_of(start + (place(levels[depth]) ^ m) * rows, SUB), rows)

    base = [sum(level[1] - 1 for level in levels[:d]) for d in range(3)]

    def scatter(g, depth, m):
        i = base[depth] + m - 1
        return pltpu.make_async_remote_copy(
            src_ref=p_ref.at[part(g, depth, m)],
            dst_ref=slot(g, depth, m),
            send_sem=send_sem.at[g, 0, i],
            recv_sem=recv_sem.at[g, 0, i],
            device_id=member(levels[depth], m),
            device_id_type=MESH,
        )

    def slot(g, depth, m):
        n = SUMMED[g][1] * NB
        at, rows = 0, n
        for d, level in enumerate(levels[:depth + 1]):
            rows //= level[1]
            if d < depth:
                at += rows * (level[1] - 1)
        return got[g].at[pl.ds(at + rows * (m - 1), rows)]

    def gather(g, depth, m):
        i = base[depth] + m - 1
        return pltpu.make_async_remote_copy(
            src_ref=p_ref.at[part(g, depth, 0)],
            dst_ref=p_ref.at[part(g, depth, 0)],
            send_sem=send_sem.at[g, 1, i],
            recv_sem=recv_sem.at[g, 1, i],
            device_id=member(levels[depth], m),
            device_id_type=MESH,
        )

    def start(kind, g, depth):
        if kind is gather:
            pl.semaphore_wait(free_sem.at[g, depth], levels[depth][1] - 1)
        for m in range(1, levels[depth][1]):
            kind(g, depth, m).start()

    def finish(kind, g, depth):
        for m in range(1, levels[depth][1]):
            kind(g, depth, m).wait()
        if kind is scatter:
            for m in range(1, levels[depth][1]):
                pl.semaphore_signal(free_sem.at[g, depth], inc=1, device_id=member(levels[depth], m), device_id_type=MESH)
            rows = part(g, depth, 0)
            total = p_ref[rows]
            for m in range(1, levels[depth][1]):
                total = total + slot(g, depth, m)[...]
            p_ref[rows] = total

    def stage(g, s):
        order = [(scatter, 0), (scatter, 1), (scatter, 2), (gather, 2), (gather, 1), (gather, 0)]
        if s > 0:
            kind, depth = order[s - 1]
            finish(kind, g, depth)
        if s < len(order):
            kind, depth = order[s]
            start(kind, g, depth)

    for c in range(CHUNKS):
        own(c).start()
    for p in range(AHEAD):
        for m in range(1, ways):
            travel(p, m).start()

    def step(p, carry):
        c, r = p // PIECES, lax.rem(p, PIECES)
        for m in range(1, ways):
            travel(p, m).wait()

        @pl.when(p + AHEAD < steps)
        def _():
            for m in range(1, ways):
                travel(p + AHEAD, m).start()

        @pl.when(r == 0)
        def _():
            own(c).wait()
            moment[...] = jnp.zeros_like(moment)

        new = load(c, r)
        for i, x in enumerate(split3(new)):
            right[i] = x
        weight = b_ref[pl.ds(pl.multiple_of(r * piece, SUB), piece), :]
        moment[...] += jnp.sum(new * weight, axis=0, keepdims=True)
        corner = lax.div(c * (c + 1), 2)

        def product(j, inner):
            left = split3(load(j, r).T)
            total = None
            for a, b in ((0, 2), (2, 0), (1, 1), (0, 1), (1, 0), (0, 0)):
                term = dot_cat(left[a], right[b])
                total = term if total is None else total + term
            rows = pl.ds(pl.multiple_of((corner + j) * NB, NB), NB)

            @pl.when(r == 0)
            def _():
                p_ref[rows] = total

            @pl.when(r > 0)
            def _():
                p_ref[rows] = p_ref[rows] + total
            return inner

        lax.fori_loop(0, c + 1, product, 0)

        @pl.when(r == PIECES - 1)
        def _():
            last = (corner + c + 1) * NB - SUB
            rows = pl.ds(pl.multiple_of(last, SUB), SUB)
            half = NB // 2
            tail = p_ref[rows, :half]
            row = lax.broadcasted_iota(jnp.int32, tail.shape, 0)
            tail = jnp.where(row == SUB - 2, moment[:, :half], tail)
            p_ref[rows, :half] = jnp.where(row == SUB - 1, moment[:, half:], tail)

        for g, ready in enumerate(READY):
            for s in range(7):
                if ready + s < steps:
                    @pl.when(p == ready + s)
                    def _(g=g, s=s):
                        stage(g, s)
        return carry

    lax.fori_loop(0, steps, step, 0)
    for g, ready in enumerate(READY):
        for s in range(7):
            if ready + s >= steps:
                stage(g, s)


def sweep(design_blk, target_col, tp_ways, dp_ways):
    levels = ladder(tp_ways, dp_ways)
    sub_rows = design_blk.shape[0] // tp_ways
    piece = sub_rows // PIECES
    blocks = CHUNKS * (CHUNKS + 1) // 2
    steps = CHUNKS * PIECES
    peers = sum(level[1] - 1 for level in levels)

    def landing(n):
        rows, total = n * NB, 0
        for level in levels:
            rows //= level[1]
            total += rows * (level[1] - 1)
        return pltpu.VMEM((total, NB), F32)

    return pl.pallas_call(
        functools.partial(sweep_kernel, levels),
        out_shape=jax.ShapeDtypeStruct((blocks * NB, NB), F32),
        in_specs=[pl.BlockSpec(memory_space=pl.ANY), pl.BlockSpec(memory_space=pltpu.VMEM)],
        out_specs=pl.BlockSpec(memory_space=pltpu.VMEM),
        scratch_shapes=[
            pltpu.VMEM((CHUNKS, tp_ways, sub_rows, NB // tp_ways), F32),
            pltpu.VMEM((3, piece, NB), BF16),
            pltpu.VMEM((1, NB), F32),
            *(landing(n) for _, n in SUMMED),
            pltpu.SemaphoreType.DMA((steps, tp_ways - 1)),
            pltpu.SemaphoreType.DMA((steps, tp_ways - 1)),
            pltpu.SemaphoreType.DMA((CHUNKS,)),
            pltpu.SemaphoreType.DMA((len(SUMMED), 2, peers)),
            pltpu.SemaphoreType.DMA((len(SUMMED), 2, peers)),
            pltpu.SemaphoreType.REGULAR((len(SUMMED), len(levels))),
        ],
        compiler_params=pltpu.CompilerParams(collective_id=0, has_side_effects=True, vmem_limit_bytes=60 * 1024 * 1024),
        cost_estimate=pl.CostEstimate(flops=300_000_000_000, bytes_accessed=32_000_000, transcendentals=0),
        name="sweep",
    )(design_blk, target_col)


def swap(x, axis, ways, mask):
    return lax.ppermute(x, axis, [(i, i ^ mask) for i in range(ways)])


def pick(stack, i):
    return lax.dynamic_index_in_dim(stack, i, 0, keepdims=False)


def scatter_sum(x, me, ways, send):
    parts = x.reshape(ways, -1, x.shape[1])
    total = pick(parts, me)
    for m in range(1, ways):
        total = total + send(pick(parts, me ^ m), m)
    return total


def gather(x, me, ways, send):
    out = jnp.zeros((ways * x.shape[0], x.shape[1]), x.dtype)
    for m in range(ways):
        out = lax.dynamic_update_slice(out, send(x, m) if m else x, ((me ^ m) * x.shape[0], 0))
    return out


def sum_all(x, tp_ways, dp_ways):
    tp, dp = lax.axis_index('tp'), lax.axis_index('dp')
    core = (dp & 1, 2, lambda v, m: swap(v, 'dp', dp_ways, m))
    plane = (dp >> 1, dp_ways // 2, lambda v, m: swap(v, 'dp', dp_ways, 2 * m))
    column = (tp, tp_ways, lambda v, m: swap(v, 'tp', tp_ways, m))
    with jax.named_scope("scatter"):
        for level in (core, plane, column):
            x = scatter_sum(x, *level)
    with jax.named_scope("gather"):
        for level in (column, plane, core):
            x = gather(x, *level)
    return x


def solution(mesh):
    tp_ways, dp_ways = mesh.shape['tp'], mesh.shape['dp']

    def local_fit(design_blk, target_blk, ridge):
        rows_dev, cols_dev = design_blk.shape
        sub_rows = rows_dev // tp_ways
        width = NB // tp_ways
        tp = lax.axis_index('tp')
        target_part = lax.dynamic_slice_in_dim(target_blk, tp * sub_rows, sub_rows)
        parts = sweep(design_blk, target_part[:, None], tp_ways, dp_ways)

        uppers, inverses, moments = {}, [], []
        for c in range(CHUNKS):
            first = NB * (c * (c + 1) // 2)
            total = parts[first:first + NB * (c + 1)]
            if c == CHUNKS - 1:
                with jax.named_scope("last_sum"):
                    total = sum_all(total, tp_ways, dp_ways)
            with jax.named_scope(f"chol{c}"):
                moments.append(total[-2:, :NB // 2].reshape(1, NB))
                for k in range(c + 1):
                    block = total[NB * k:NB * (k + 1)]
                    for j in range(k):
                        block = block - gram(uppers[j, k], uppers[j, c])
                    if k < c:
                        uppers[k, c] = jnp.dot(inverses[k], block, precision=HIGHEST, preferred_element_type=F32)
                    else:
                        inverses.append(diag_inverse(block, ridge))
        with jax.named_scope("solve"):
            order = solve(jnp.concatenate(moments, axis=0), uppers, inverses)
            order = order.reshape(CHUNKS, tp_ways, width)
            coeffs = order.transpose(1, 0, 2).reshape(-1)
            coeff_blk = lax.dynamic_index_in_dim(order, tp, 1, keepdims=False).reshape(-1)
        with jax.named_scope("fit"):
            fitted = jnp.sum(design_blk * coeff_blk[None, :], axis=1)
            for k in range(tp_ways.bit_length() - 1):
                fitted = fitted + swap(fitted, 'tp', tp_ways, 1 << k)
        return coeffs, target_blk - fitted

    return jax.shard_map(local_fit, mesh=mesh, in_specs=(P('dp', 'tp'), P('dp'), P()), out_specs=(P(), P('dp')), check_vma=False)
```

```python
import functools

import jax
import jax.numpy as jnp
from jax import lax
from jax.experimental import pallas as pl
from jax.experimental.pallas import tpu as pltpu
from jax.sharding import PartitionSpec as P


LANES = 128
SUB = 8
BLK = 128
NB = 512
CHUNKS = 5
MESH = pl.DeviceIdType.MESH
F32 = jnp.float32
BF16 = jnp.bfloat16


def split3(x):
    hi = x.astype(BF16)
    rest = x - hi.astype(F32)
    mid = rest.astype(BF16)
    low = (rest - mid.astype(F32)).astype(BF16)
    return hi, mid, low


def lhs_cat(x):
    hi, mid, low = split3(x)
    return jnp.concatenate([hi, mid, hi, low, mid, hi], axis=1)


def rhs_cat(x):
    hi, mid, low = split3(x)
    return jnp.concatenate([mid, hi, low, hi, mid, hi], axis=0)


def dot_cat(lhs, rhs):
    return lax.dot_general(lhs, rhs, (((1,), (0,)), ((), ())), preferred_element_type=F32)


def row_sums(parts, sub):
    for shift in (4, 2, 1):
        low = (sub & shift) == 0
        nxt = []
        for t in range(shift):
            a, b = parts[t], parts[t + shift]
            keep = jnp.where(low, a, b)
            move = jnp.where(low, b, a)
            nxt.append(keep + xor_roll(move, shift, sub))
        parts = nxt
    return parts[0]


def xor_roll(x, shift, sub):
    if shift == 4:
        return pltpu.roll(x, 4, 0)
    low = (sub & shift) == 0
    return jnp.where(low, pltpu.roll(x, SUB - shift, 0), pltpu.roll(x, shift, 0))


def bcast_lane(x, c):
    return jnp.broadcast_to(x[:, c:c + 1], (SUB, LANES))


def bcast_row(x, p):
    return jnp.broadcast_to(x[p:p + 1, :], (SUB, LANES))


def factor_block(load, sub, lane):
    octs = BLK // SUB
    a = [load(o) for o in range(octs)]
    e = [jnp.where(lane == sub + SUB * o, 1.0, 0.0).astype(F32) for o in range(octs)]
    out = [None] * octs
    for t in range(octs // 2):
        o0, o1 = 2 * t, 2 * t + 1
        c0 = 16 * t
        r0, r1, e0, e1 = a[o0], a[o1], e[o0], e[o1]
        b0 = [bcast_lane(r0, c0 + q) for q in range(16)]
        b1 = [bcast_lane(r1, c0 + q) for q in range(16)]
        d0 = jnp.ones((SUB, LANES), F32)
        d1 = jnp.ones((SUB, LANES), F32)
        for p in range(16):
            ps = p % 8
            first = p < 8
            piv = bcast_row(b0[p] if first else b1[p], ps)
            inv = 1.0 / piv
            if first:
                d0 = jnp.where(sub == ps, piv, d0)
                m0 = jnp.where(sub > ps, b0[p] * inv, 0.0)
                m1 = b1[p] * inv
            else:
                d1 = jnp.where(sub == ps, piv, d1)
                m1 = jnp.where(sub > ps, b1[p] * inv, 0.0)
            for q in range(p + 1, 16):
                row = bcast_row(b0[q] if first else b1[q], ps)
                if first and ps < 7:
                    b0[q] = b0[q] - m0 * row
                b1[q] = b1[q] - m1 * row
            rr, re = bcast_row(r0 if first else r1, ps), bcast_row(e0 if first else e1, ps)
            if first and ps < 7:
                r0 = r0 - m0 * rr
                e0 = e0 - m0 * re
            r1 = r1 - m1 * rr
            e1 = e1 - m1 * re
        s0, s1 = lax.rsqrt(d0), lax.rsqrt(d1)
        u0, u1, v0, v1 = r0 * s0, r1 * s1, e0 * s0, e1 * s1
        out[o0], out[o1] = v0, v1
        for o in range(2 * t + 2, octs):
            xs, ys = [], []
            for k in range(SUB):
                i = SUB * o + k
                g0, g1 = bcast_lane(u0, i), bcast_lane(u1, i)
                xs.append(g0 * u0 + g1 * u1)
                ys.append(g0 * v0 + g1 * v1)
            a[o] = a[o] - row_sums(xs, sub)
            e[o] = e[o] - row_sums(ys, sub)
    return out


def diag_kernel(lam_ref, s_ref, w_ref, work):
    n = s_ref.shape[0]
    steps = n // BLK
    sub = lax.broadcasted_iota(jnp.int32, (SUB, LANES), 0)
    lane = lax.broadcasted_iota(jnp.int32, (SUB, LANES), 1)
    row = lax.broadcasted_iota(jnp.int32, (n, n), 0)
    col = lax.broadcasted_iota(jnp.int32, (n, n), 1)
    work[:, :n] = s_ref[...] + jnp.where(row == col, lam_ref[0], 0.0)
    work[:, n:] = jnp.where(row == col, 1.0, 0.0)

    def step(k, carry):
        base = pl.multiple_of(k * BLK, BLK)
        win = pl.ds(pl.multiple_of(base + BLK, BLK), n)
        diag = pl.ds(base, BLK)

        def load(o):
            return work[pl.ds(pl.multiple_of(base + SUB * o, SUB), SUB), diag]

        inv = jnp.concatenate(factor_block(load, sub, lane), axis=0)
        panel = dot_cat(lhs_cat(inv), rhs_cat(work[diag, win]))
        work[diag, win] = panel
        right = rhs_cat(panel)
        for j in range(steps - 1):
            @pl.when(k == j)
            def _(j=j):
                rows = n - BLK * (j + 1)
                left = lhs_cat(panel[:, :rows].T)
                w = (pl.ds(BLK * (j + 1), rows), pl.ds(BLK * (j + 1), n))
                work[w] = work[w] - dot_cat(left, right)
        return carry

    lax.fori_loop(0, steps, step, 0)
    w_ref[...] = work[:, n:]


def diag_inverse(sdiag, lam):
    n = sdiag.shape[0]
    return pl.pallas_call(
        diag_kernel,
        out_shape=jax.ShapeDtypeStruct((n, n), F32),
        in_specs=[pl.BlockSpec(memory_space=pltpu.SMEM), pl.BlockSpec(memory_space=pltpu.VMEM)],
        out_specs=pl.BlockSpec(memory_space=pltpu.VMEM),
        scratch_shapes=[pltpu.VMEM((n, 2 * n), F32)],
        cost_estimate=pl.CostEstimate(flops=20_000_000_000, bytes_accessed=8 * n * n, transcendentals=0),
        name="diag_inverse",
    )(lam.reshape(1), sdiag)


def finish_kernel(ways, h_ref, b_ref, a_hbm, *refs):
    n, pairs = CHUNKS, [(j, c) for c in range(CHUNKS) for j in range(c)]
    blocks = len(pairs) + n
    hbm = refs[:blocks]
    x_ref, r_ref, near, a_ref, fit, load_sem, a_sem, send_sem, recv_sem = refs[blocks:]
    nb = near.shape[1]
    rows_dev = a_ref.shape[0]
    loads = [pltpu.make_async_copy(ref, near.at[i], load_sem.at[i]) for i, ref in enumerate(hbm)]
    quarter = rows_dev // a_sem.shape[0]
    spans = [pl.ds(quarter * i, quarter) for i in range(a_sem.shape[0])]
    fetch = [pltpu.make_async_copy(a_hbm.at[span], a_ref.at[span], a_sem.at[i]) for i, span in enumerate(spans)]
    order = [pairs.index((j, c)) if j < c else len(pairs) + c for c in range(n) for j in range(c + 1)]
    for i in order:
        loads[i].start()
    for copy in fetch:
        copy.start()
    z = lax.axis_index("tp")
    barrier = pltpu.get_barrier_semaphore()
    for m in range(1, ways):
        pl.semaphore_signal(barrier, inc=1, device_id={"tp": z ^ m}, device_id_type=MESH)
    pl.semaphore_wait(barrier, ways - 1)

    def upper(j, c):
        return near[pairs.index((j, c))]

    half = []
    for c in range(n):
        right = h_ref[c:c + 1, :]
        for j in range(c):
            loads[pairs.index((j, c))].wait()
            right = right - jnp.sum(upper(j, c) * half[j], axis=0, keepdims=True)
        loads[len(pairs) + c].wait()
        half.append(jnp.sum(near[len(pairs) + c] * right, axis=1, keepdims=True))
    for c in reversed(range(n)):
        left = half[c]
        for k in range(c + 1, n):
            left = left - jnp.sum(upper(c, k) * x_ref[k:k + 1, :], axis=1, keepdims=True)
        x_ref[c:c + 1, :] = jnp.sum(near[len(pairs) + c] * left, axis=0, keepdims=True)

    width = nb // ways
    lanes = pl.ds(pl.multiple_of(z * width, LANES), width)
    mine = [x_ref[c:c + 1, lanes] for c in range(n)]

    def product(i, carry):
        rows = pl.ds(pl.multiple_of(i * BLK, BLK), BLK)
        terms = [a_ref[rows, width * c:width * (c + 1)] * mine[c] for c in range(n)]
        total = terms[0]
        for term in terms[1:]:
            total = total + term
        fit[z, pl.ds(i, 1), :] = jnp.sum(total.T, axis=0, keepdims=True)
        return carry

    for i, copy in enumerate(fetch):
        copy.wait()
        lax.fori_loop(quarter // BLK * i, quarter // BLK * (i + 1), product, 0)
    copies = [
        pltpu.make_async_remote_copy(
            src_ref=fit.at[z], dst_ref=fit.at[z], send_sem=send_sem.at[m - 1], recv_sem=recv_sem.at[m - 1],
            device_id={"tp": z ^ m}, device_id_type=MESH)
        for m in range(1, ways)
    ]
    for copy in copies:
        copy.start()
    for copy in copies:
        copy.wait()
    total = fit[0]
    for t in range(1, ways):
        total = total + fit[t]
    r_ref[...] = b_ref[...] - total


def finish(moment, target_blk, design_blk, uppers, inverses, ways):
    blocks = [uppers[j, c] for c in range(CHUNKS) for j in range(c)] + inverses
    rows_dev, cols_dev = design_blk.shape
    vmem, hbm = pl.BlockSpec(memory_space=pltpu.VMEM), pl.BlockSpec(memory_space=pl.ANY)
    return pl.pallas_call(
        functools.partial(finish_kernel, ways),
        out_shape=(jax.ShapeDtypeStruct((CHUNKS, NB), F32), jax.ShapeDtypeStruct((rows_dev // LANES, LANES), F32)),
        in_specs=[vmem, vmem, hbm] + [hbm] * len(blocks),
        out_specs=(vmem, vmem),
        scratch_shapes=[
            pltpu.VMEM((len(blocks), NB, NB), F32),
            pltpu.VMEM((rows_dev, cols_dev), F32),
            pltpu.VMEM((ways, rows_dev // LANES, LANES), F32),
            pltpu.SemaphoreType.DMA((len(blocks),)),
            pltpu.SemaphoreType.DMA((4,)),
            pltpu.SemaphoreType.DMA((ways - 1,)),
            pltpu.SemaphoreType.DMA((ways - 1,)),
        ],
        compiler_params=pltpu.CompilerParams(collective_id=1, has_side_effects=True, vmem_limit_bytes=48 * 1024 * 1024),
        cost_estimate=pl.CostEstimate(flops=5_000_000_000, bytes_accessed=32_000_000, transcendentals=0),
        name="finish",
    )(moment, target_blk.reshape(-1, LANES), design_blk, *blocks)


HIGHEST = lax.Precision.HIGHEST
CONTRACT_ROWS = (((0,), (0,)), ((), ()))


def gram(left, right):
    return lax.dot_general(left, right, CONTRACT_ROWS, precision=HIGHEST, preferred_element_type=F32)


PIECES = 3
AHEAD = 2
SUMMED = ((0, 3), (3, 3), (6, 4))
OUTS = 11
WHEN = ((5, 6, 7, 9, 11, 12, 13), (8, 9, 10, 12, 14, 15, 16), (11, 12, 13, 15, 16, 17, 18))


def ladder(tp_ways, dp_ways):
    return (("dp", 2, 1), ("dp", dp_ways // 2, 2), ("tp", tp_ways, 1))


def place(level):
    axis, ways, dist = level
    return lax.rem(lax.axis_index(axis) // dist, ways)


def member(level, m):
    axis, _, dist = level
    return {axis: lax.axis_index(axis) ^ (m * dist)}


def sweep_kernel(levels, a_ref, b_ref, *refs):
    outs, (p_ref, x_ref, right, moment, got0, got1, got2, swap_send, swap_recv, own_sem, send_sem, recv_sem, free_sem, out_sem) = refs[:OUTS], refs[OUTS:]
    ways = levels[2][1]
    sub_rows = a_ref.shape[0] // ways
    width = a_ref.shape[1] // CHUNKS
    piece = sub_rows // PIECES
    steps = CHUNKS * PIECES
    z = lax.axis_index("tp")
    got = (got0, got1, got2)

    barrier = pltpu.get_barrier_semaphore()
    count = 0
    for level in levels:
        for m in range(1, level[1]):
            pl.semaphore_signal(barrier, inc=1, device_id=member(level, m), device_id_type=MESH)
            count += 1
    pl.semaphore_wait(barrier, count)

    def own(c):
        return pltpu.make_async_copy(
            a_ref.at[pl.ds(z * sub_rows, sub_rows), pl.ds(width * c, width)], x_ref.at[c, z], own_sem.at[c])

    def travel(p, m):
        c, r = p // PIECES, lax.rem(p, PIECES)
        rows = pl.ds(pl.multiple_of((z ^ m) * sub_rows + r * piece, SUB), piece)
        cols = pl.ds(pl.multiple_of(c * width, LANES), width)
        return pltpu.make_async_remote_copy(
            src_ref=a_ref.at[rows, cols],
            dst_ref=x_ref.at[c, z, pl.ds(pl.multiple_of(r * piece, SUB), piece)],
            send_sem=swap_send.at[p, m - 1],
            recv_sem=swap_recv.at[p, m - 1],
            device_id=member(levels[2], m),
            device_id_type=MESH,
        )

    def load(c, r):
        rows = pl.ds(pl.multiple_of(r * piece, SUB), piece)
        return jnp.concatenate([x_ref[c, t, rows, :] for t in range(ways)], axis=1)

    def span(g, depth):
        first, n = SUMMED[g]
        start, rows = first * NB, n * NB
        for level in levels[:depth]:
            rows //= level[1]
            start = start + place(level) * rows
        return start, rows

    def part(g, depth, m):
        start, _ = span(g, depth)
        rows = span(g, depth + 1)[1]
        return pl.ds(pl.multiple_of(start + (place(levels[depth]) ^ m) * rows, SUB), rows)

    base = [sum(level[1] - 1 for level in levels[:d]) for d in range(3)]

    def scatter(g, depth, m):
        i = base[depth] + m - 1
        return pltpu.make_async_remote_copy(
            src_ref=p_ref.at[part(g, depth, m)],
            dst_ref=slot(g, depth, m),
            send_sem=send_sem.at[g, 0, i],
            recv_sem=recv_sem.at[g, 0, i],
            device_id=member(levels[depth], m),
            device_id_type=MESH,
        )

    def slot(g, depth, m):
        n = SUMMED[g][1] * NB
        at, rows = 0, n
        for d, level in enumerate(levels[:depth + 1]):
            rows //= level[1]
            if d < depth:
                at += rows * (level[1] - 1)
        return got[g].at[pl.ds(at + rows * (m - 1), rows)]

    def gather(g, depth, m):
        i = base[depth] + m - 1
        return pltpu.make_async_remote_copy(
            src_ref=p_ref.at[part(g, depth, 0)],
            dst_ref=p_ref.at[part(g, depth, 0)],
            send_sem=send_sem.at[g, 1, i],
            recv_sem=recv_sem.at[g, 1, i],
            device_id=member(levels[depth], m),
            device_id_type=MESH,
        )

    def start(kind, g, depth):
        if kind is gather:
            pl.semaphore_wait(free_sem.at[g, depth], levels[depth][1] - 1)
        for m in range(1, levels[depth][1]):
            kind(g, depth, m).start()

    def finish(kind, g, depth):
        for m in range(1, levels[depth][1]):
            kind(g, depth, m).wait()
        if kind is scatter:
            for m in range(1, levels[depth][1]):
                pl.semaphore_signal(free_sem.at[g, depth], inc=1, device_id=member(levels[depth], m), device_id_type=MESH)
            rows = part(g, depth, 0)
            total = p_ref[rows]
            for m in range(1, levels[depth][1]):
                total = total + slot(g, depth, m)[...]
            p_ref[rows] = total

    def stage(g, s):
        order = [(scatter, 0), (scatter, 1), (scatter, 2), (gather, 2), (gather, 1), (gather, 0)]
        if s > 0:
            kind, depth = order[s - 1]
            finish(kind, g, depth)
        if s < len(order):
            kind, depth = order[s]
            start(kind, g, depth)
        else:
            first, n = SUMMED[g]
            for i in range(first, first + n):
                leave(i).start()

    def leave(i):
        rows = pl.ds(NB * i, NB) if i < OUTS - 1 else pl.ds(NB * i, p_ref.shape[0] - NB * i)
        return pltpu.make_async_copy(p_ref.at[rows], outs[i], out_sem.at[i])

    def stages(p, first):
        for g, when in enumerate(WHEN):
            for s, w in enumerate(when):
                if w < steps and (s == 0) == first:
                    @pl.when(p == w)
                    def _(g=g, s=s):
                        stage(g, s)

    for c in range(CHUNKS):
        own(c).start()
    for p in range(AHEAD):
        for m in range(1, ways):
            travel(p, m).start()

    def step(p, carry):
        c, r = p // PIECES, lax.rem(p, PIECES)
        for m in range(1, ways):
            travel(p, m).wait()

        @pl.when(p + AHEAD < steps)
        def _():
            for m in range(1, ways):
                travel(p + AHEAD, m).start()

        @pl.when(r == 0)
        def _():
            own(c).wait()
            moment[...] = jnp.zeros_like(moment)

        stages(p, False)
        new = load(c, r)
        for i, x in enumerate(split3(new)):
            right[i] = x
        weight = b_ref[pl.ds(pl.multiple_of(r * piece, SUB), piece), :]
        moment[...] += jnp.sum(new * weight, axis=0, keepdims=True)
        corner = lax.div(c * (c + 1), 2)

        def product(j, inner):
            left = split3(load(j, r).T)
            total = None
            for a, b in ((0, 2), (2, 0), (1, 1), (0, 1), (1, 0), (0, 0)):
                term = dot_cat(left[a], right[b])
                total = term if total is None else total + term
            rows = pl.ds(pl.multiple_of((corner + j) * NB, NB), NB)

            @pl.when(r == 0)
            def _():
                p_ref[rows] = total

            @pl.when(r > 0)
            def _():
                p_ref[rows] = p_ref[rows] + total

            return inner

        lax.fori_loop(0, c + 1, product, 0)

        @pl.when(r == PIECES - 1)
        def _():
            last = (corner + c + 1) * NB - SUB
            rows = pl.ds(pl.multiple_of(last, SUB), SUB)
            half = NB // 2
            tail = p_ref[rows, :half]
            row = lax.broadcasted_iota(jnp.int32, tail.shape, 0)
            tail = jnp.where(row == SUB - 2, moment[:, :half], tail)
            p_ref[rows, :half] = jnp.where(row == SUB - 1, moment[:, half:], tail)

        stages(p, True)
        return carry

    lax.fori_loop(0, steps, step, 0)
    leave(OUTS - 1).start()
    for p in range(steps, max(WHEN[-1]) + 1):
        for g, when in enumerate(WHEN):
            for s, w in enumerate(when):
                if w == p:
                    stage(g, s)
    for i in range(OUTS):
        leave(i).wait()


def sweep(design_blk, target_col, tp_ways, dp_ways):
    levels = ladder(tp_ways, dp_ways)
    sub_rows = design_blk.shape[0] // tp_ways
    piece = sub_rows // PIECES
    blocks = CHUNKS * (CHUNKS + 1) // 2
    steps = CHUNKS * PIECES
    peers = sum(level[1] - 1 for level in levels)

    def landing(n):
        rows, total = n * NB, 0
        for level in levels:
            rows //= level[1]
            total += rows * (level[1] - 1)
        return pltpu.VMEM((total, NB), F32)

    return pl.pallas_call(
        functools.partial(sweep_kernel, levels),
        out_shape=[jax.ShapeDtypeStruct((NB, NB), F32)] * (OUTS - 1) + [jax.ShapeDtypeStruct((CHUNKS * NB, NB), F32)],
        in_specs=[pl.BlockSpec(memory_space=pl.ANY), pl.BlockSpec(memory_space=pltpu.VMEM)],
        out_specs=[pl.BlockSpec(memory_space=pl.ANY)] * OUTS,
        scratch_shapes=[
            pltpu.VMEM((blocks * NB, NB), F32),
            pltpu.VMEM((CHUNKS, tp_ways, sub_rows, NB // tp_ways), F32),
            pltpu.VMEM((3, piece, NB), BF16),
            pltpu.VMEM((1, NB), F32),
            *(landing(n) for _, n in SUMMED),
            pltpu.SemaphoreType.DMA((steps, tp_ways - 1)),
            pltpu.SemaphoreType.DMA((steps, tp_ways - 1)),
            pltpu.SemaphoreType.DMA((CHUNKS,)),
            pltpu.SemaphoreType.DMA((len(SUMMED), 2, peers)),
            pltpu.SemaphoreType.DMA((len(SUMMED), 2, peers)),
            pltpu.SemaphoreType.REGULAR((len(SUMMED), len(levels))),
            pltpu.SemaphoreType.DMA((OUTS,)),
        ],
        compiler_params=pltpu.CompilerParams(collective_id=0, has_side_effects=True, vmem_limit_bytes=60 * 1024 * 1024),
        cost_estimate=pl.CostEstimate(flops=300_000_000_000, bytes_accessed=32_000_000, transcendentals=0),
        name="sweep",
    )(design_blk, target_col)


def swap(x, axis, ways, mask):
    return lax.ppermute(x, axis, [(i, i ^ mask) for i in range(ways)])


def pick(stack, i):
    return lax.dynamic_index_in_dim(stack, i, 0, keepdims=False)


def scatter_sum(x, me, ways, send):
    parts = x.reshape(ways, -1, x.shape[1])
    total = pick(parts, me)
    for m in range(1, ways):
        total = total + send(pick(parts, me ^ m), m)
    return total


def gather(x, me, ways, send):
    out = jnp.zeros((ways * x.shape[0], x.shape[1]), x.dtype)
    for m in range(ways):
        out = lax.dynamic_update_slice(out, send(x, m) if m else x, ((me ^ m) * x.shape[0], 0))
    return out


def sum_all(x, tp_ways, dp_ways):
    tp, dp = lax.axis_index('tp'), lax.axis_index('dp')
    core = (dp & 1, 2, lambda v, m: swap(v, 'dp', dp_ways, m))
    plane = (dp >> 1, dp_ways // 2, lambda v, m: swap(v, 'dp', dp_ways, 2 * m))
    column = (tp, tp_ways, lambda v, m: swap(v, 'tp', tp_ways, m))
    for level in (core, plane, column):
        x = scatter_sum(x, *level)
    for level in (column, plane, core):
        x = gather(x, *level)
    return x


def solution(mesh):
    tp_ways, dp_ways = mesh.shape['tp'], mesh.shape['dp']

    def local_fit(design_blk, target_blk, ridge):
        rows_dev, _ = design_blk.shape
        sub_rows = rows_dev // tp_ways
        width = NB // tp_ways
        tp = lax.axis_index('tp')
        target_part = lax.dynamic_slice_in_dim(target_blk, tp * sub_rows, sub_rows)
        *blocks, last = sweep(design_blk, target_part[:, None], tp_ways, dp_ways)
        last = sum_all(last, tp_ways, dp_ways)
        blocks += [last[NB * k:NB * (k + 1)] for k in range(CHUNKS)]

        uppers, inverses, moments = {}, [], []
        for c in range(CHUNKS):
            total = blocks[c * (c + 1) // 2:]
            moments.append(total[c][-2:, :NB // 2].reshape(1, NB))
            for k in range(c + 1):
                block = total[k]
                for j in range(k):
                    block = block - gram(uppers[j, k], uppers[j, c])
                if k < c:
                    uppers[k, c] = jnp.dot(inverses[k], block, precision=HIGHEST, preferred_element_type=F32)
                else:
                    inverses.append(diag_inverse(block, ridge))
        order, residual = finish(jnp.concatenate(moments, axis=0), target_blk, design_blk, uppers, inverses, tp_ways)
        coeffs = order.reshape(CHUNKS, tp_ways, width).transpose(1, 0, 2).reshape(-1)
        return coeffs, residual.reshape(-1)

    return jax.shard_map(local_fit, mesh=mesh, in_specs=(P('dp', 'tp'), P('dp'), P()), out_specs=(P(), P('dp')), check_vma=False)
```

```python
import functools

import jax
import jax.numpy as jnp
from jax import lax
from jax.experimental import pallas as pl
from jax.experimental.pallas import tpu as pltpu
from jax.sharding import PartitionSpec as P


LANES = 128
SUB = 8
BLK = 128
NB = 512
CHUNKS = 5
MESH = pl.DeviceIdType.MESH
F32 = jnp.float32
BF16 = jnp.bfloat16


def split3(x):
    hi = x.astype(BF16)
    rest = x - hi.astype(F32)
    mid = rest.astype(BF16)
    low = (rest - mid.astype(F32)).astype(BF16)
    return hi, mid, low


def lhs_cat(x):
    hi, mid, low = split3(x)
    return jnp.concatenate([hi, mid, hi, low, mid, hi], axis=1)


def rhs_cat(x):
    hi, mid, low = split3(x)
    return jnp.concatenate([mid, hi, low, hi, mid, hi], axis=0)


def dot_cat(lhs, rhs):
    return lax.dot_general(lhs, rhs, (((1,), (0,)), ((), ())), preferred_element_type=F32)


def row_sums(parts, sub):
    for shift in (4, 2, 1):
        low = (sub & shift) == 0
        nxt = []
        for t in range(shift):
            a, b = parts[t], parts[t + shift]
            keep = jnp.where(low, a, b)
            move = jnp.where(low, b, a)
            nxt.append(keep + xor_roll(move, shift, sub))
        parts = nxt
    return parts[0]


def xor_roll(x, shift, sub):
    if shift == 4:
        return pltpu.roll(x, 4, 0)
    low = (sub & shift) == 0
    return jnp.where(low, pltpu.roll(x, SUB - shift, 0), pltpu.roll(x, shift, 0))


def bcast_lane(x, c):
    return jnp.broadcast_to(x[:, c:c + 1], (SUB, LANES))


def bcast_row(x, p):
    return jnp.broadcast_to(x[p:p + 1, :], (SUB, LANES))


def factor_block(load, sub, lane):
    octs = BLK // SUB
    a = [load(o) for o in range(octs)]
    e = [jnp.where(lane == sub + SUB * o, 1.0, 0.0).astype(F32) for o in range(octs)]
    out = [None] * octs
    for t in range(octs // 2):
        o0, o1 = 2 * t, 2 * t + 1
        c0 = 16 * t
        r0, r1, e0, e1 = a[o0], a[o1], e[o0], e[o1]
        b0 = [bcast_lane(r0, c0 + q) for q in range(16)]
        b1 = [bcast_lane(r1, c0 + q) for q in range(16)]
        d0 = jnp.ones((SUB, LANES), F32)
        d1 = jnp.ones((SUB, LANES), F32)
        for p in range(16):
            ps = p % 8
            first = p < 8
            piv = bcast_row(b0[p] if first else b1[p], ps)
            inv = 1.0 / piv
            if first:
                d0 = jnp.where(sub == ps, piv, d0)
                m0 = jnp.where(sub > ps, b0[p] * inv, 0.0)
                m1 = b1[p] * inv
            else:
                d1 = jnp.where(sub == ps, piv, d1)
                m1 = jnp.where(sub > ps, b1[p] * inv, 0.0)
            for q in range(p + 1, 16):
                row = bcast_row(b0[q] if first else b1[q], ps)
                if first and ps < 7:
                    b0[q] = b0[q] - m0 * row
                b1[q] = b1[q] - m1 * row
            rr, re = bcast_row(r0 if first else r1, ps), bcast_row(e0 if first else e1, ps)
            if first and ps < 7:
                r0 = r0 - m0 * rr
                e0 = e0 - m0 * re
            r1 = r1 - m1 * rr
            e1 = e1 - m1 * re
        s0, s1 = lax.rsqrt(d0), lax.rsqrt(d1)
        u0, u1, v0, v1 = r0 * s0, r1 * s1, e0 * s0, e1 * s1
        out[o0], out[o1] = v0, v1
        for o in range(2 * t + 2, octs):
            xs, ys = [], []
            for k in range(SUB):
                i = SUB * o + k
                g0, g1 = bcast_lane(u0, i), bcast_lane(u1, i)
                xs.append(g0 * u0 + g1 * u1)
                ys.append(g0 * v0 + g1 * v1)
            a[o] = a[o] - row_sums(xs, sub)
            e[o] = e[o] - row_sums(ys, sub)
    return out


def diag_kernel(lam_ref, s_ref, w_ref, work):
    n = s_ref.shape[0]
    steps = n // BLK
    sub = lax.broadcasted_iota(jnp.int32, (SUB, LANES), 0)
    lane = lax.broadcasted_iota(jnp.int32, (SUB, LANES), 1)
    row = lax.broadcasted_iota(jnp.int32, (n, n), 0)
    col = lax.broadcasted_iota(jnp.int32, (n, n), 1)
    work[:, :n] = s_ref[...] + jnp.where(row == col, lam_ref[0], 0.0)
    work[:, n:] = jnp.where(row == col, 1.0, 0.0)

    def step(k, carry):
        base = pl.multiple_of(k * BLK, BLK)
        win = pl.ds(pl.multiple_of(base + BLK, BLK), n)
        diag = pl.ds(base, BLK)

        def load(o):
            return work[pl.ds(pl.multiple_of(base + SUB * o, SUB), SUB), diag]

        inv = jnp.concatenate(factor_block(load, sub, lane), axis=0)
        panel = dot_cat(lhs_cat(inv), rhs_cat(work[diag, win]))
        work[diag, win] = panel
        right = rhs_cat(panel)
        for j in range(steps - 1):
            @pl.when(k == j)
            def _(j=j):
                rows = n - BLK * (j + 1)
                left = lhs_cat(panel[:, :rows].T)
                w = (pl.ds(BLK * (j + 1), rows), pl.ds(BLK * (j + 1), n))
                work[w] = work[w] - dot_cat(left, right)
        return carry

    lax.fori_loop(0, steps, step, 0)
    w_ref[...] = work[:, n:]


def diag_inverse(panel, lam):
    n = panel.shape[0]
    return pl.pallas_call(
        diag_kernel,
        out_shape=jax.ShapeDtypeStruct((n, n), F32),
        grid=(1,),
        in_specs=[pl.BlockSpec(memory_space=pltpu.SMEM), pl.BlockSpec((n, n), lambda i: (0, 0))],
        out_specs=pl.BlockSpec((n, n), lambda i: (0, 0)),
        scratch_shapes=[pltpu.VMEM((n, 2 * n), F32)],
        cost_estimate=pl.CostEstimate(flops=20_000_000_000, bytes_accessed=8 * n * n, transcendentals=0),
        name="diag_inverse",
    )(lam.reshape(1), panel)


def finish_kernel(ways, h_ref, b_ref, a_hbm, *refs):
    n, pairs = CHUNKS, [(j, c) for c in range(CHUNKS) for j in range(c)]
    panels, tops, inverses, refs = refs[:LAST - 1], refs[LAST - 1:2 * LAST - 1], refs[2 * LAST - 1:3 * LAST], refs[3 * LAST:]
    x_ref, r_ref, near, a_ref, fit, load_sem, a_sem, send_sem, recv_sem = refs
    hbm = [tops[j] if c == LAST else panels[j].at[:, pl.ds(NB * (c - j - 1), NB)] for j, c in pairs] + list(inverses)
    nb = near.shape[1]
    rows_dev = a_ref.shape[0]
    loads = [pltpu.make_async_copy(ref, near.at[i], load_sem.at[i]) for i, ref in enumerate(hbm)]
    quarter = rows_dev // a_sem.shape[0]
    spans = [pl.ds(quarter * i, quarter) for i in range(a_sem.shape[0])]
    fetch = [pltpu.make_async_copy(a_hbm.at[span], a_ref.at[span], a_sem.at[i]) for i, span in enumerate(spans)]
    order = [pairs.index((j, c)) if j < c else len(pairs) + c for c in range(n) for j in range(c + 1)]
    for i in order:
        loads[i].start()
    for copy in fetch:
        copy.start()
    z = lax.axis_index("tp")
    barrier = pltpu.get_barrier_semaphore()
    for m in range(1, ways):
        pl.semaphore_signal(barrier, inc=1, device_id={"tp": z ^ m}, device_id_type=MESH)
    pl.semaphore_wait(barrier, ways - 1)

    def upper(j, c):
        return near[pairs.index((j, c))]

    half = []
    for c in range(n):
        right = h_ref[c:c + 1, :]
        for j in range(c):
            loads[pairs.index((j, c))].wait()
            right = right - jnp.sum(upper(j, c) * half[j], axis=0, keepdims=True)
        loads[len(pairs) + c].wait()
        half.append(jnp.sum(near[len(pairs) + c] * right, axis=1, keepdims=True))
    for c in reversed(range(n)):
        left = half[c]
        for k in range(c + 1, n):
            left = left - jnp.sum(upper(c, k) * x_ref[k:k + 1, :], axis=1, keepdims=True)
        x_ref[c:c + 1, :] = jnp.sum(near[len(pairs) + c] * left, axis=0, keepdims=True)

    width = nb // ways
    lanes = pl.ds(pl.multiple_of(z * width, LANES), width)
    mine = [x_ref[c:c + 1, lanes] for c in range(n)]

    def product(i, carry):
        for k in range(group):
            at = i * group + k
            rows = pl.ds(pl.multiple_of(at * BLK, BLK), BLK)
            terms = [a_ref[rows, width * c:width * (c + 1)] * mine[c] for c in range(n)]
            total = terms[0]
            for term in terms[1:]:
                total = total + term
            fit[z, pl.ds(at, 1), :] = jnp.sum(total.T, axis=0, keepdims=True)
        return carry

    group = 4 if quarter % (4 * BLK) == 0 else 1
    for i, copy in enumerate(fetch):
        copy.wait()
        lax.fori_loop(quarter // (group * BLK) * i, quarter // (group * BLK) * (i + 1), product, 0)
    copies = [
        pltpu.make_async_remote_copy(
            src_ref=fit.at[z], dst_ref=fit.at[z], send_sem=send_sem.at[m - 1], recv_sem=recv_sem.at[m - 1],
            device_id={"tp": z ^ m}, device_id_type=MESH)
        for m in range(1, ways)
    ]
    for copy in copies:
        copy.start()
    for copy in copies:
        copy.wait()
    total = fit[0]
    for t in range(1, ways):
        total = total + fit[t]
    r_ref[...] = b_ref[...] - total


def finish(moment, target_blk, design_blk, uppers, tops, inverses, ways):
    blocks = CHUNKS * (CHUNKS + 1) // 2
    parts = [*uppers, *tops, *inverses]
    rows_dev, cols_dev = design_blk.shape
    vmem, hbm = pl.BlockSpec(memory_space=pltpu.VMEM), pl.BlockSpec(memory_space=pl.ANY)
    return pl.pallas_call(
        functools.partial(finish_kernel, ways),
        out_shape=(jax.ShapeDtypeStruct((CHUNKS, NB), F32), jax.ShapeDtypeStruct((rows_dev // LANES, LANES), F32)),
        in_specs=[vmem, vmem, hbm] + [hbm] * len(parts),
        out_specs=(vmem, vmem),
        scratch_shapes=[
            pltpu.VMEM((blocks, NB, NB), F32),
            pltpu.VMEM((rows_dev, cols_dev), F32),
            pltpu.VMEM((ways, rows_dev // LANES, LANES), F32),
            pltpu.SemaphoreType.DMA((blocks,)),
            pltpu.SemaphoreType.DMA((4,)),
            pltpu.SemaphoreType.DMA((ways - 1,)),
            pltpu.SemaphoreType.DMA((ways - 1,)),
        ],
        compiler_params=pltpu.CompilerParams(collective_id=1, has_side_effects=True, vmem_limit_bytes=48 * 1024 * 1024),
        cost_estimate=pl.CostEstimate(flops=5_000_000_000, bytes_accessed=32_000_000, transcendentals=0),
        name="finish",
    )(moment, target_blk.reshape(-1, LANES), design_blk, *parts)


HIGHEST = lax.Precision.HIGHEST
CONTRACT_ROWS = (((0,), (0,)), ((), ()))


def gram(left, right):
    return lax.dot_general(left, right, CONTRACT_ROWS, precision=HIGHEST, preferred_element_type=F32)


PIECES = 6
AHEAD = 2
LAST = CHUNKS - 1
PANELS = LAST
SUMMED = ((0, 3), (3, 3), (6, 4), (10, 5))
WHEN = (
    (11, 12, 14, 16, 18, 20, 22, 24, 25),
    (17, 18, 20, 22, 24, 26, 28, 30, 31),
    (23, 24, 26, 28, 30, 31, 32, 33, 34),
    (29, 30),
)


def ladder(tp_ways, dp_ways):
    pairs = tuple(("tp", 2, 1 << k) for k in range(tp_ways.bit_length() - 1))
    return (("dp", 2, 1), ("dp", dp_ways // 2, 2), *pairs)


def steps_of(levels, g):
    if g == len(SUMMED) - 1:
        return [(False, 0)]
    depths = range(len(levels))
    return [(False, d) for d in depths] + [(True, d) for d in reversed(depths)]


def place(level):
    axis, ways, dist = level
    return lax.rem(lax.axis_index(axis) // dist, ways)


def member(level, m):
    axis, _, dist = level
    return {axis: lax.axis_index(axis) ^ (m * dist)}


def sweep_kernel(levels, ways, a_ref, b_ref, *refs):
    outs, (p_ref, x_ref, right, moment, *got) = refs[:PANELS + 1], refs[PANELS + 1:]
    swap_send, swap_recv, own_sem, send_sem, recv_sem, free_sem, out_sem = got[len(SUMMED):]
    sub_rows = a_ref.shape[0] // ways
    width = a_ref.shape[1] // CHUNKS
    piece = sub_rows // PIECES
    steps = CHUNKS * PIECES
    z = lax.axis_index("tp")
    column = ("tp", ways, 1)

    barrier = pltpu.get_barrier_semaphore()
    count = 0
    for level in (*levels[:2], column):
        for m in range(1, level[1]):
            pl.semaphore_signal(barrier, inc=1, device_id=member(level, m), device_id_type=MESH)
            count += 1
    pl.semaphore_wait(barrier, count)

    def own(c):
        return pltpu.make_async_copy(
            a_ref.at[pl.ds(z * sub_rows, sub_rows), pl.ds(width * c, width)], x_ref.at[c, z], own_sem.at[c])

    def travel(p, m):
        c, r = p // PIECES, lax.rem(p, PIECES)
        rows = pl.ds(pl.multiple_of((z ^ m) * sub_rows + r * piece, SUB), piece)
        cols = pl.ds(pl.multiple_of(c * width, LANES), width)
        return pltpu.make_async_remote_copy(
            src_ref=a_ref.at[rows, cols],
            dst_ref=x_ref.at[c, z, pl.ds(pl.multiple_of(r * piece, SUB), piece)],
            send_sem=swap_send.at[p, m - 1],
            recv_sem=swap_recv.at[p, m - 1],
            device_id=member(column, m),
            device_id_type=MESH,
        )

    def load(c, r):
        rows = pl.ds(pl.multiple_of(r * piece, SUB), piece)
        return jnp.concatenate([x_ref[c, t, rows, :] for t in range(ways)], axis=1)

    def span(g, depth):
        first, n = SUMMED[g]
        start, rows = first * NB, n * NB
        for level in levels[:depth]:
            rows //= level[1]
            start = start + place(level) * rows
        return start, rows

    def part(g, depth, m):
        start, _ = span(g, depth)
        rows = span(g, depth + 1)[1]
        return pl.ds(pl.multiple_of(start + (place(levels[depth]) ^ m) * rows, SUB), rows)

    base = [sum(level[1] - 1 for level in levels[:d]) for d in range(len(levels))]

    def scatter(g, depth, m):
        i = base[depth] + m - 1
        return pltpu.make_async_remote_copy(
            src_ref=p_ref.at[part(g, depth, m)],
            dst_ref=slot(g, depth, m),
            send_sem=send_sem.at[g, 0, i],
            recv_sem=recv_sem.at[g, 0, i],
            device_id=member(levels[depth], m),
            device_id_type=MESH,
        )

    def slot(g, depth, m):
        n = SUMMED[g][1] * NB
        at, rows = 0, n
        for d, level in enumerate(levels[:depth + 1]):
            rows //= level[1]
            if d < depth:
                at += rows * (level[1] - 1)
        return got[g].at[pl.ds(at + rows * (m - 1), rows)]

    def gather(g, depth, m):
        i = base[depth] + m - 1
        return pltpu.make_async_remote_copy(
            src_ref=p_ref.at[part(g, depth, 0)],
            dst_ref=p_ref.at[part(g, depth, 0)],
            send_sem=send_sem.at[g, 1, i],
            recv_sem=recv_sem.at[g, 1, i],
            device_id=member(levels[depth], m),
            device_id_type=MESH,
        )

    def start(back, g, depth):
        if back:
            pl.semaphore_wait(free_sem.at[g, depth], levels[depth][1] - 1)
        for m in range(1, levels[depth][1]):
            (gather if back else scatter)(g, depth, m).start()

    def finish(back, g, depth):
        others = range(1, levels[depth][1])
        for m in others:
            (gather if back else scatter)(g, depth, m).wait()
        if back:
            return
        if (True, depth) in steps_of(levels, g):
            for m in others:
                pl.semaphore_signal(free_sem.at[g, depth], inc=1, device_id=member(levels[depth], m), device_id_type=MESH)
        rows = part(g, depth, 0)
        total = p_ref[rows]
        for m in others:
            total = total + slot(g, depth, m)[...]
        p_ref[rows] = total

    def leave(i):
        c = max(c for c in range(CHUNKS) if c * (c + 1) // 2 <= i)
        k = i - c * (c + 1) // 2
        return pltpu.make_async_copy(
            p_ref.at[pl.ds(NB * i, NB)], outs[k].at[:, pl.ds(NB * (c - k), NB)], out_sem.at[i])

    def leave_last():
        return pltpu.make_async_copy(p_ref.at[part(len(SUMMED) - 1, 0, 0)], outs[PANELS], out_sem.at[SUMMED[-1][0]])

    def stage(g, s):
        order = steps_of(levels, g)
        if s > 0:
            finish(*order[s - 1][:1], g, order[s - 1][1])
        if s < len(order):
            start(order[s][0], g, order[s][1])
        elif g == len(SUMMED) - 1:
            leave_last().start()
        else:
            first, n = SUMMED[g]
            for i in range(first, first + n):
                leave(i).start()

    def stages(p, first):
        for g, when in enumerate(WHEN):
            for s, w in enumerate(when):
                if w < steps and (s == 0) == first:
                    @pl.when(p == w)
                    def _(g=g, s=s):
                        stage(g, s)

    for c in range(CHUNKS):
        own(c).start()
    for p in range(AHEAD):
        for m in range(1, ways):
            travel(p, m).start()

    def step(p, carry):
        c, r = p // PIECES, lax.rem(p, PIECES)
        for m in range(1, ways):
            travel(p, m).wait()

        @pl.when(p + AHEAD < steps)
        def _():
            for m in range(1, ways):
                travel(p + AHEAD, m).start()

        @pl.when(r == 0)
        def _():
            own(c).wait()
            moment[...] = jnp.zeros_like(moment)

        stages(p, False)
        new = load(c, r)
        for i, x in enumerate(split3(new)):
            right[i] = x
        weight = b_ref[pl.ds(pl.multiple_of(r * piece, SUB), piece), :]
        moment[...] += jnp.sum(new * weight, axis=0, keepdims=True)
        corner = lax.div(c * (c + 1), 2)

        def product(j, inner):
            left = split3(load(j, r).T)
            total = None
            for a, b in ((0, 2), (2, 0), (1, 1), (0, 1), (1, 0), (0, 0)):
                term = dot_cat(left[a], right[b])
                total = term if total is None else total + term
            rows = pl.ds(pl.multiple_of((corner + j) * NB, NB), NB)

            @pl.when(r == 0)
            def _():
                p_ref[rows] = total

            @pl.when(r > 0)
            def _():
                p_ref[rows] = p_ref[rows] + total

            return inner

        lax.fori_loop(0, c + 1, product, 0)

        @pl.when(r == PIECES - 1)
        def _():
            last = (corner + c + 1) * NB - SUB
            rows = pl.ds(pl.multiple_of(last, SUB), SUB)
            half = NB // 2
            tail = p_ref[rows, :half]
            row = lax.broadcasted_iota(jnp.int32, tail.shape, 0)
            tail = jnp.where(row == SUB - 2, moment[:, :half], tail)
            p_ref[rows, :half] = jnp.where(row == SUB - 1, moment[:, half:], tail)

        stages(p, True)
        return carry

    lax.fori_loop(0, steps, step, 0)
    for p in range(steps, max(w for when in WHEN for w in when) + 1):
        for g, when in enumerate(WHEN):
            for s, w in enumerate(when):
                if w == p:
                    stage(g, s)
    for i in range(SUMMED[-1][0]):
        leave(i).wait()
    leave_last().wait()


def sweep(design_blk, target_col, tp_ways, dp_ways):
    levels = ladder(tp_ways, dp_ways)
    sub_rows = design_blk.shape[0] // tp_ways
    piece = sub_rows // PIECES
    blocks = CHUNKS * (CHUNKS + 1) // 2
    steps = CHUNKS * PIECES
    peers = sum(level[1] - 1 for level in levels)

    def landing(g):
        rows, total = SUMMED[g][1] * NB, 0
        for back, depth in steps_of(levels, g):
            if not back:
                rows //= levels[depth][1]
                total += rows * (levels[depth][1] - 1)
        return pltpu.VMEM((total, NB), F32)

    return pl.pallas_call(
        functools.partial(sweep_kernel, levels, tp_ways),
        out_shape=[jax.ShapeDtypeStruct((NB, NB * (LAST - k)), F32) for k in range(PANELS)]
        + [jax.ShapeDtypeStruct((CHUNKS * NB // 2, NB), F32)],
        in_specs=[pl.BlockSpec(memory_space=pl.ANY), pl.BlockSpec(memory_space=pltpu.VMEM)],
        out_specs=[pl.BlockSpec(memory_space=pl.ANY)] * (PANELS + 1),
        scratch_shapes=[
            pltpu.VMEM((blocks * NB, NB), F32),
            pltpu.VMEM((CHUNKS, tp_ways, sub_rows, NB // tp_ways), F32),
            pltpu.VMEM((3, piece, NB), BF16),
            pltpu.VMEM((1, NB), F32),
            *(landing(g) for g in range(len(SUMMED))),
            pltpu.SemaphoreType.DMA((steps, tp_ways - 1)),
            pltpu.SemaphoreType.DMA((steps, tp_ways - 1)),
            pltpu.SemaphoreType.DMA((CHUNKS,)),
            pltpu.SemaphoreType.DMA((len(SUMMED), 2, peers)),
            pltpu.SemaphoreType.DMA((len(SUMMED), 2, peers)),
            pltpu.SemaphoreType.REGULAR((len(SUMMED), len(levels))),
            pltpu.SemaphoreType.DMA((SUMMED[-1][0] + 1,)),
        ],
        compiler_params=pltpu.CompilerParams(collective_id=0, has_side_effects=True, vmem_limit_bytes=60 * 1024 * 1024),
        cost_estimate=pl.CostEstimate(flops=300_000_000_000, bytes_accessed=32_000_000, transcendentals=0),
        name="sweep",
    )(design_blk, target_col)


def swap(x, axis, ways, mask):
    return lax.ppermute(x, axis, [(i, i ^ mask) for i in range(ways)])


def pick(stack, i):
    return lax.dynamic_index_in_dim(stack, i, 0, keepdims=False)


def scatter_sum(x, me, ways, send):
    parts = x.reshape(ways, -1, x.shape[1])
    total = pick(parts, me)
    for m in range(1, ways):
        total = total + send(pick(parts, me ^ m), m)
    return total


def gather(x, me, ways, send):
    out = jnp.zeros((ways * x.shape[0], x.shape[1]), x.dtype)
    for m in range(ways):
        out = lax.dynamic_update_slice(out, send(x, m) if m else x, ((me ^ m) * x.shape[0], 0))
    return out


def sum_rest(x, tp_ways, dp_ways):
    tp, dp = lax.axis_index('tp'), lax.axis_index('dp')
    core = (dp & 1, 2, lambda v, m: swap(v, 'dp', dp_ways, m))
    plane = (dp >> 1, dp_ways // 2, lambda v, m: swap(v, 'dp', dp_ways, 2 * m))
    column = (tp, tp_ways, lambda v, m: swap(v, 'tp', tp_ways, m))
    for level in (plane, column):
        x = scatter_sum(x, *level)
    for level in (column, plane, core):
        x = gather(x, *level)
    return x


def solution(mesh):
    tp_ways, dp_ways = mesh.shape['tp'], mesh.shape['dp']

    def local_fit(design_blk, target_blk, ridge):
        rows_dev, _ = design_blk.shape
        sub_rows = rows_dev // tp_ways
        width = NB // tp_ways
        tp = lax.axis_index('tp')
        target_part = lax.dynamic_slice_in_dim(target_blk, tp * sub_rows, sub_rows)
        *panels, last = sweep(design_blk, target_part[:, None], tp_ways, dp_ways)
        last = sum_rest(last, tp_ways, dp_ways)
        moments = [panel[NB - 2:, :NB // 2] for panel in panels] + [last[-2:, :NB // 2]]

        uppers, tops, inverses = [], [], []
        for k in range(PANELS):
            inverses.append(diag_inverse(panels[k], ridge))
            if k < PANELS - 1:
                upper = jnp.dot(inverses[k], panels[k][:, NB:], precision=HIGHEST, preferred_element_type=F32)
                uppers.append(upper)
                for r in range(k + 1, PANELS):
                    at = NB * (r - k - 1)
                    panels[r] = panels[r] - gram(upper[:, at:at + NB], upper[:, at:])
        corner = last[NB * LAST:]
        rest = last[:NB * LAST]
        for k in range(PANELS):
            tops.append(jnp.dot(inverses[k], rest[:NB], precision=HIGHEST, preferred_element_type=F32))
            if k < PANELS - 1:
                rest = rest[NB:] - gram(uppers[k], tops[k])
            corner = corner - gram(tops[k], tops[k])
        inverses.append(diag_inverse(corner, ridge))
        moment = jnp.concatenate([m.reshape(1, NB) for m in moments], axis=0)
        order, residual = finish(moment, target_blk, design_blk, uppers, tops, inverses, tp_ways)
        coeffs = order.reshape(CHUNKS, tp_ways, width).transpose(1, 0, 2).reshape(-1)
        return coeffs, residual.reshape(-1)

    return jax.shard_map(local_fit, mesh=mesh, in_specs=(P('dp', 'tp'), P('dp'), P()), out_specs=(P(), P('dp')), check_vma=False)
```

```python
import functools

import jax
import jax.numpy as jnp
from jax import lax
from jax.experimental import pallas as pl
from jax.experimental.pallas import tpu as pltpu
from jax.sharding import PartitionSpec as P


LANES = 128
SUB = 8
BLK = 128
NB = 512
CHUNKS = 5
MESH = pl.DeviceIdType.MESH
F32 = jnp.float32
BF16 = jnp.bfloat16


def split3(x):
    hi = x.astype(BF16)
    rest = x - hi.astype(F32)
    mid = rest.astype(BF16)
    low = (rest - mid.astype(F32)).astype(BF16)
    return hi, mid, low


def lhs_cat(x):
    hi, mid, low = split3(x)
    return jnp.concatenate([hi, mid, hi, low, mid, hi], axis=1)


def rhs_cat(x):
    hi, mid, low = split3(x)
    return jnp.concatenate([mid, hi, low, hi, mid, hi], axis=0)


def dot_cat(lhs, rhs):
    return lax.dot_general(lhs, rhs, (((1,), (0,)), ((), ())), preferred_element_type=F32)


def row_sums(parts, sub):
    for shift in (4, 2, 1):
        low = (sub & shift) == 0
        nxt = []
        for t in range(shift):
            a, b = parts[t], parts[t + shift]
            keep = jnp.where(low, a, b)
            move = jnp.where(low, b, a)
            nxt.append(keep + xor_roll(move, shift, sub))
        parts = nxt
    return parts[0]


def xor_roll(x, shift, sub):
    if shift == 4:
        return pltpu.roll(x, 4, 0)
    low = (sub & shift) == 0
    return jnp.where(low, pltpu.roll(x, SUB - shift, 0), pltpu.roll(x, shift, 0))


def bcast_lane(x, c):
    return jnp.broadcast_to(x[:, c:c + 1], (SUB, LANES))


def bcast_row(x, p):
    return jnp.broadcast_to(x[p:p + 1, :], (SUB, LANES))


def factor_block(load, sub, lane):
    octs = BLK // SUB
    a = [load(o) for o in range(octs)]
    e = [jnp.where(lane == sub + SUB * o, 1.0, 0.0).astype(F32) for o in range(octs)]
    out = [None] * octs
    for t in range(octs // 2):
        o0, o1 = 2 * t, 2 * t + 1
        c0 = 16 * t
        r0, r1, e0, e1 = a[o0], a[o1], e[o0], e[o1]
        b0 = [bcast_lane(r0, c0 + q) for q in range(16)]
        b1 = [bcast_lane(r1, c0 + q) for q in range(16)]
        d0 = jnp.ones((SUB, LANES), F32)
        d1 = jnp.ones((SUB, LANES), F32)
        for p in range(16):
            ps = p % 8
            first = p < 8
            piv = bcast_row(b0[p] if first else b1[p], ps)
            inv = 1.0 / piv
            if first:
                d0 = jnp.where(sub == ps, piv, d0)
                m0 = jnp.where(sub > ps, b0[p] * inv, 0.0)
                m1 = b1[p] * inv
            else:
                d1 = jnp.where(sub == ps, piv, d1)
                m1 = jnp.where(sub > ps, b1[p] * inv, 0.0)
            for q in range(p + 1, 16):
                row = bcast_row(b0[q] if first else b1[q], ps)
                if first and ps < 7:
                    b0[q] = b0[q] - m0 * row
                b1[q] = b1[q] - m1 * row
            rr, re = bcast_row(r0 if first else r1, ps), bcast_row(e0 if first else e1, ps)
            if first and ps < 7:
                r0 = r0 - m0 * rr
                e0 = e0 - m0 * re
            r1 = r1 - m1 * rr
            e1 = e1 - m1 * re
        s0, s1 = lax.rsqrt(d0), lax.rsqrt(d1)
        u0, u1, v0, v1 = r0 * s0, r1 * s1, e0 * s0, e1 * s1
        out[o0], out[o1] = v0, v1
        for o in range(2 * t + 2, octs):
            xs, ys = [], []
            for k in range(SUB):
                i = SUB * o + k
                g0, g1 = bcast_lane(u0, i), bcast_lane(u1, i)
                xs.append(g0 * u0 + g1 * u1)
                ys.append(g0 * v0 + g1 * v1)
            a[o] = a[o] - row_sums(xs, sub)
            e[o] = e[o] - row_sums(ys, sub)
    return out


def diag_kernel(lam_ref, s_ref, w_ref, work):
    n = s_ref.shape[0]
    steps = n // BLK
    sub = lax.broadcasted_iota(jnp.int32, (SUB, LANES), 0)
    lane = lax.broadcasted_iota(jnp.int32, (SUB, LANES), 1)
    row = lax.broadcasted_iota(jnp.int32, (n, n), 0)
    col = lax.broadcasted_iota(jnp.int32, (n, n), 1)
    work[:, :n] = s_ref[...] + jnp.where(row == col, lam_ref[0], 0.0)
    work[:, n:] = jnp.where(row == col, 1.0, 0.0)

    def step(k, carry):
        base = pl.multiple_of(k * BLK, BLK)
        win = pl.ds(pl.multiple_of(base + BLK, BLK), n)
        diag = pl.ds(base, BLK)

        def load(o):
            return work[pl.ds(pl.multiple_of(base + SUB * o, SUB), SUB), diag]

        inv = jnp.concatenate(factor_block(load, sub, lane), axis=0)
        panel = dot_cat(lhs_cat(inv), rhs_cat(work[diag, win]))
        work[diag, win] = panel
        right = rhs_cat(panel)
        for j in range(steps - 1):
            @pl.when(k == j)
            def _(j=j):
                rows = n - BLK * (j + 1)
                left = lhs_cat(panel[:, :rows].T)
                w = (pl.ds(BLK * (j + 1), rows), pl.ds(BLK * (j + 1), n))
                work[w] = work[w] - dot_cat(left, right)
        return carry

    lax.fori_loop(0, steps, step, 0)
    w_ref[...] = work[:, n:]


def diag_inverse(panel, lam):
    n = panel.shape[0]
    return pl.pallas_call(
        diag_kernel,
        out_shape=jax.ShapeDtypeStruct((n, n), F32),
        grid=(1,),
        in_specs=[pl.BlockSpec(memory_space=pltpu.SMEM), pl.BlockSpec((n, n), lambda i: (0, 0))],
        out_specs=pl.BlockSpec((n, n), lambda i: (0, 0)),
        scratch_shapes=[pltpu.VMEM((n, 2 * n), F32)],
        cost_estimate=pl.CostEstimate(flops=20_000_000_000, bytes_accessed=8 * n * n, transcendentals=0),
        name="diag_inverse",
    )(lam.reshape(1), panel)


def finish_kernel(ways, h_ref, b_ref, a_hbm, *refs):
    n, pairs = CHUNKS, [(j, c) for c in range(CHUNKS) for j in range(c)]
    panels, tops, inverses, refs = refs[:LAST - 1], refs[LAST - 1:2 * LAST - 1], refs[2 * LAST - 1:3 * LAST], refs[3 * LAST:]
    x_ref, r_ref, near, a_ref, fit, load_sem, a_sem, send_sem, recv_sem = refs
    hbm = [tops[j] if c == LAST else panels[j].at[:, pl.ds(NB * (c - j - 1), NB)] for j, c in pairs] + list(inverses)
    nb = near.shape[1]
    rows_dev = a_ref.shape[0]
    loads = [pltpu.make_async_copy(ref, near.at[i], load_sem.at[i]) for i, ref in enumerate(hbm)]
    quarter = rows_dev // a_sem.shape[0]
    spans = [pl.ds(quarter * i, quarter) for i in range(a_sem.shape[0])]
    fetch = [pltpu.make_async_copy(a_hbm.at[span], a_ref.at[span], a_sem.at[i]) for i, span in enumerate(spans)]
    order = [pairs.index((j, c)) if j < c else len(pairs) + c for c in range(n) for j in range(c + 1)]
    for i in order:
        loads[i].start()
    for copy in fetch:
        copy.start()
    z = lax.axis_index("tp")
    barrier = pltpu.get_barrier_semaphore()
    for m in range(1, ways):
        pl.semaphore_signal(barrier, inc=1, device_id={"tp": z ^ m}, device_id_type=MESH)
    pl.semaphore_wait(barrier, ways - 1)

    def upper(j, c):
        return near[pairs.index((j, c))]

    half = []
    for c in range(n):
        right = h_ref[c:c + 1, :]
        for j in range(c):
            loads[pairs.index((j, c))].wait()
            right = right - jnp.sum(upper(j, c) * half[j], axis=0, keepdims=True)
        loads[len(pairs) + c].wait()
        half.append(jnp.sum(near[len(pairs) + c] * right, axis=1, keepdims=True))
    for c in reversed(range(n)):
        left = half[c]
        for k in range(c + 1, n):
            left = left - jnp.sum(upper(c, k) * x_ref[k:k + 1, :], axis=1, keepdims=True)
        x_ref[c:c + 1, :] = jnp.sum(near[len(pairs) + c] * left, axis=0, keepdims=True)

    width = nb // ways
    lanes = pl.ds(pl.multiple_of(z * width, LANES), width)
    mine = [x_ref[c:c + 1, lanes] for c in range(n)]

    def product(i, carry):
        for k in range(group):
            at = i * group + k
            rows = pl.ds(pl.multiple_of(at * BLK, BLK), BLK)
            terms = [a_ref[rows, width * c:width * (c + 1)] * mine[c] for c in range(n)]
            total = terms[0]
            for term in terms[1:]:
                total = total + term
            fit[z, pl.ds(at, 1), :] = jnp.sum(total.T, axis=0, keepdims=True)
        return carry

    group = 4 if quarter % (4 * BLK) == 0 else 1
    for i, copy in enumerate(fetch):
        copy.wait()
        lax.fori_loop(quarter // (group * BLK) * i, quarter // (group * BLK) * (i + 1), product, 0)
    copies = [
        pltpu.make_async_remote_copy(
            src_ref=fit.at[z], dst_ref=fit.at[z], send_sem=send_sem.at[m - 1], recv_sem=recv_sem.at[m - 1],
            device_id={"tp": z ^ m}, device_id_type=MESH)
        for m in range(1, ways)
    ]
    for copy in copies:
        copy.start()
    for copy in copies:
        copy.wait()
    total = fit[0]
    for t in range(1, ways):
        total = total + fit[t]
    r_ref[...] = b_ref[...] - total


def finish(moment, target_blk, design_blk, uppers, tops, inverses, ways):
    blocks = CHUNKS * (CHUNKS + 1) // 2
    parts = [*uppers, *tops, *inverses]
    rows_dev, cols_dev = design_blk.shape
    vmem, hbm = pl.BlockSpec(memory_space=pltpu.VMEM), pl.BlockSpec(memory_space=pl.ANY)
    return pl.pallas_call(
        functools.partial(finish_kernel, ways),
        out_shape=(jax.ShapeDtypeStruct((CHUNKS, NB), F32), jax.ShapeDtypeStruct((rows_dev // LANES, LANES), F32)),
        in_specs=[vmem, vmem, hbm] + [hbm] * len(parts),
        out_specs=(vmem, vmem),
        scratch_shapes=[
            pltpu.VMEM((blocks, NB, NB), F32),
            pltpu.VMEM((rows_dev, cols_dev), F32),
            pltpu.VMEM((ways, rows_dev // LANES, LANES), F32),
            pltpu.SemaphoreType.DMA((blocks,)),
            pltpu.SemaphoreType.DMA((4,)),
            pltpu.SemaphoreType.DMA((ways - 1,)),
            pltpu.SemaphoreType.DMA((ways - 1,)),
        ],
        compiler_params=pltpu.CompilerParams(collective_id=1, has_side_effects=True, vmem_limit_bytes=48 * 1024 * 1024),
        cost_estimate=pl.CostEstimate(flops=5_000_000_000, bytes_accessed=32_000_000, transcendentals=0),
        name="finish",
    )(moment, target_blk.reshape(-1, LANES), design_blk, *parts)


HIGHEST = lax.Precision.HIGHEST
CONTRACT_ROWS = (((0,), (0,)), ((), ()))


def gram(left, right):
    return lax.dot_general(left, right, CONTRACT_ROWS, precision=HIGHEST, preferred_element_type=F32)


PIECES = 6
AHEAD = 2
LAST = CHUNKS - 1
PANELS = LAST
SUMMED = ((0, 3), (3, 3), (6, 4), (10, 5))
WHEN = (
    (11, 12, 14, 15, 16, 17, 18, 20, 21),
    (17, 18, 21, 22, 23, 24, 26, 28, 29),
    (23, 24, 26, 27, 28, 29, 30, 31, 32),
    (29, 30),
)


def ladder(tp_ways, dp_ways):
    pairs = tuple(("tp", 2, 1 << k) for k in range(tp_ways.bit_length() - 1))
    return (("dp", 2, 1), ("dp", dp_ways // 2, 2), *pairs)


def steps_of(levels, g):
    if g == len(SUMMED) - 1:
        return [(False, 0)]
    depths = range(len(levels))
    return [(False, d) for d in depths] + [(True, d) for d in reversed(depths)]


def place(level):
    axis, ways, dist = level
    return lax.rem(lax.axis_index(axis) // dist, ways)


def member(level, m):
    axis, _, dist = level
    return {axis: lax.axis_index(axis) ^ (m * dist)}


def sweep_kernel(levels, ways, a_ref, b_ref, *refs):
    outs, (p_ref, x_ref, right, moment, *got) = refs[:PANELS + 1], refs[PANELS + 1:]
    swap_send, swap_recv, own_sem, send_sem, recv_sem, free_sem, out_sem = got[len(SUMMED):]
    sub_rows = a_ref.shape[0] // ways
    width = a_ref.shape[1] // CHUNKS
    piece = sub_rows // PIECES
    steps = CHUNKS * PIECES
    z = lax.axis_index("tp")
    column = ("tp", ways, 1)

    barrier = pltpu.get_barrier_semaphore()
    count = 0
    for level in (*levels[:2], column):
        for m in range(1, level[1]):
            pl.semaphore_signal(barrier, inc=1, device_id=member(level, m), device_id_type=MESH)
            count += 1
    pl.semaphore_wait(barrier, count)

    def own(c):
        return pltpu.make_async_copy(
            a_ref.at[pl.ds(z * sub_rows, sub_rows), pl.ds(width * c, width)], x_ref.at[c, z], own_sem.at[c])

    def travel(p, m):
        c, r = p // PIECES, lax.rem(p, PIECES)
        rows = pl.ds(pl.multiple_of((z ^ m) * sub_rows + r * piece, SUB), piece)
        cols = pl.ds(pl.multiple_of(c * width, LANES), width)
        return pltpu.make_async_remote_copy(
            src_ref=a_ref.at[rows, cols],
            dst_ref=x_ref.at[c, z, pl.ds(pl.multiple_of(r * piece, SUB), piece)],
            send_sem=swap_send.at[p, m - 1],
            recv_sem=swap_recv.at[p, m - 1],
            device_id=member(column, m),
            device_id_type=MESH,
        )

    def load(c, r):
        rows = pl.ds(pl.multiple_of(r * piece, SUB), piece)
        return jnp.concatenate([x_ref[c, t, rows, :] for t in range(ways)], axis=1)

    def span(g, depth):
        first, n = SUMMED[g]
        start, rows = first * NB, n * NB
        for level in levels[:depth]:
            rows //= level[1]
            start = start + place(level) * rows
        return start, rows

    def part(g, depth, m):
        start, _ = span(g, depth)
        rows = span(g, depth + 1)[1]
        return pl.ds(pl.multiple_of(start + (place(levels[depth]) ^ m) * rows, SUB), rows)

    base = [sum(level[1] - 1 for level in levels[:d]) for d in range(len(levels))]

    def scatter(g, depth, m):
        i = base[depth] + m - 1
        return pltpu.make_async_remote_copy(
            src_ref=p_ref.at[part(g, depth, m)],
            dst_ref=slot(g, depth, m),
            send_sem=send_sem.at[g, 0, i],
            recv_sem=recv_sem.at[g, 0, i],
            device_id=member(levels[depth], m),
            device_id_type=MESH,
        )

    def slot(g, depth, m):
        n = SUMMED[g][1] * NB
        at, rows = 0, n
        for d, level in enumerate(levels[:depth + 1]):
            rows //= level[1]
            if d < depth:
                at += rows * (level[1] - 1)
        return got[g].at[pl.ds(at + rows * (m - 1), rows)]

    def gather(g, depth, m):
        i = base[depth] + m - 1
        return pltpu.make_async_remote_copy(
            src_ref=p_ref.at[part(g, depth, 0)],
            dst_ref=p_ref.at[part(g, depth, 0)],
            send_sem=send_sem.at[g, 1, i],
            recv_sem=recv_sem.at[g, 1, i],
            device_id=member(levels[depth], m),
            device_id_type=MESH,
        )

    def start(back, g, depth):
        if back:
            pl.semaphore_wait(free_sem.at[g, depth], levels[depth][1] - 1)
        for m in range(1, levels[depth][1]):
            (gather if back else scatter)(g, depth, m).start()

    def finish(back, g, depth):
        others = range(1, levels[depth][1])
        for m in others:
            (gather if back else scatter)(g, depth, m).wait()
        if back:
            return
        if (True, depth) in steps_of(levels, g):
            for m in others:
                pl.semaphore_signal(free_sem.at[g, depth], inc=1, device_id=member(levels[depth], m), device_id_type=MESH)
        rows = part(g, depth, 0)
        total = p_ref[rows]
        for m in others:
            total = total + slot(g, depth, m)[...]
        p_ref[rows] = total

    def leave(i):
        c = max(c for c in range(CHUNKS) if c * (c + 1) // 2 <= i)
        k = i - c * (c + 1) // 2
        return pltpu.make_async_copy(
            p_ref.at[pl.ds(NB * i, NB)], outs[k].at[:, pl.ds(NB * (c - k), NB)], out_sem.at[i])

    def leave_last():
        return pltpu.make_async_copy(p_ref.at[part(len(SUMMED) - 1, 0, 0)], outs[PANELS], out_sem.at[SUMMED[-1][0]])

    def stage(g, s):
        order = steps_of(levels, g)
        if s > 0:
            finish(*order[s - 1][:1], g, order[s - 1][1])
        if s < len(order):
            start(order[s][0], g, order[s][1])
        elif g == len(SUMMED) - 1:
            leave_last().start()
        else:
            first, n = SUMMED[g]
            for i in range(first, first + n):
                leave(i).start()

    def stages(p, first):
        for g, when in enumerate(WHEN):
            for s, w in enumerate(when):
                if w < steps and (s == 0) == first:
                    @pl.when(p == w)
                    def _(g=g, s=s):
                        stage(g, s)

    for c in range(CHUNKS):
        own(c).start()
    for p in range(AHEAD):
        for m in range(1, ways):
            travel(p, m).start()

    def step(p, carry):
        c, r = p // PIECES, lax.rem(p, PIECES)
        for m in range(1, ways):
            travel(p, m).wait()

        stages(p, False)

        @pl.when(p + AHEAD < steps)
        def _():
            for m in range(1, ways):
                travel(p + AHEAD, m).start()

        @pl.when(r == 0)
        def _():
            own(c).wait()
            moment[...] = jnp.zeros_like(moment)

        new = load(c, r)
        for i, x in enumerate(split3(new)):
            right[i] = x
        weight = b_ref[pl.ds(pl.multiple_of(r * piece, SUB), piece), :]
        moment[...] += jnp.sum(new * weight, axis=0, keepdims=True)
        corner = lax.div(c * (c + 1), 2)

        def product(j, inner):
            left = split3(load(j, r).T)
            total = None
            for a, b in ((0, 2), (2, 0), (1, 1), (0, 1), (1, 0), (0, 0)):
                term = dot_cat(left[a], right[b])
                total = term if total is None else total + term
            rows = pl.ds(pl.multiple_of((corner + j) * NB, NB), NB)

            @pl.when(r == 0)
            def _():
                p_ref[rows] = total

            @pl.when(r > 0)
            def _():
                p_ref[rows] = p_ref[rows] + total

            return inner

        lax.fori_loop(0, c + 1, product, 0)

        @pl.when(r == PIECES - 1)
        def _():
            last = (corner + c + 1) * NB - SUB
            rows = pl.ds(pl.multiple_of(last, SUB), SUB)
            half = NB // 2
            tail = p_ref[rows, :half]
            row = lax.broadcasted_iota(jnp.int32, tail.shape, 0)
            tail = jnp.where(row == SUB - 2, moment[:, :half], tail)
            p_ref[rows, :half] = jnp.where(row == SUB - 1, moment[:, half:], tail)

        stages(p, True)
        return carry

    lax.fori_loop(0, steps, step, 0)
    for p in range(steps, max(w for when in WHEN for w in when) + 1):
        for g, when in enumerate(WHEN):
            for s, w in enumerate(when):
                if w == p:
                    stage(g, s)
    for i in range(SUMMED[-1][0]):
        leave(i).wait()
    leave_last().wait()


def sweep(design_blk, target_col, tp_ways, dp_ways):
    levels = ladder(tp_ways, dp_ways)
    sub_rows = design_blk.shape[0] // tp_ways
    piece = sub_rows // PIECES
    blocks = CHUNKS * (CHUNKS + 1) // 2
    steps = CHUNKS * PIECES
    peers = sum(level[1] - 1 for level in levels)

    def landing(g):
        rows, total = SUMMED[g][1] * NB, 0
        for back, depth in steps_of(levels, g):
            if not back:
                rows //= levels[depth][1]
                total += rows * (levels[depth][1] - 1)
        return pltpu.VMEM((total, NB), F32)

    return pl.pallas_call(
        functools.partial(sweep_kernel, levels, tp_ways),
        out_shape=[jax.ShapeDtypeStruct((NB, NB * (LAST - k)), F32) for k in range(PANELS)]
        + [jax.ShapeDtypeStruct((CHUNKS * NB // 2, NB), F32)],
        in_specs=[pl.BlockSpec(memory_space=pl.ANY), pl.BlockSpec(memory_space=pltpu.VMEM)],
        out_specs=[pl.BlockSpec(memory_space=pl.ANY)] * (PANELS + 1),
        scratch_shapes=[
            pltpu.VMEM((blocks * NB, NB), F32),
            pltpu.VMEM((CHUNKS, tp_ways, sub_rows, NB // tp_ways), F32),
            pltpu.VMEM((3, piece, NB), BF16),
            pltpu.VMEM((1, NB), F32),
            *(landing(g) for g in range(len(SUMMED))),
            pltpu.SemaphoreType.DMA((steps, tp_ways - 1)),
            pltpu.SemaphoreType.DMA((steps, tp_ways - 1)),
            pltpu.SemaphoreType.DMA((CHUNKS,)),
            pltpu.SemaphoreType.DMA((len(SUMMED), 2, peers)),
            pltpu.SemaphoreType.DMA((len(SUMMED), 2, peers)),
            pltpu.SemaphoreType.REGULAR((len(SUMMED), len(levels))),
            pltpu.SemaphoreType.DMA((SUMMED[-1][0] + 1,)),
        ],
        compiler_params=pltpu.CompilerParams(collective_id=0, has_side_effects=True, vmem_limit_bytes=60 * 1024 * 1024),
        cost_estimate=pl.CostEstimate(flops=300_000_000_000, bytes_accessed=32_000_000, transcendentals=0),
        name="sweep",
    )(design_blk, target_col)


def swap(x, axis, ways, mask):
    return lax.ppermute(x, axis, [(i, i ^ mask) for i in range(ways)])


def pick(stack, i):
    return lax.dynamic_index_in_dim(stack, i, 0, keepdims=False)


def scatter_sum(x, me, ways, send):
    parts = x.reshape(ways, -1, x.shape[1])
    total = pick(parts, me)
    for m in range(1, ways):
        total = total + send(pick(parts, me ^ m), m)
    return total


def gather(x, me, ways, send):
    got = [x] + [send(x, m) for m in range(1, ways)]
    rows = []
    for i in range(ways):
        part = got[ways - 1]
        for m in range(ways - 1):
            part = jnp.where(me == i ^ m, got[m], part)
        rows.append(part)
    return jnp.concatenate(rows, axis=0)


def sum_rest(x, tp_ways, dp_ways):
    tp, dp = lax.axis_index('tp'), lax.axis_index('dp')
    core = (dp & 1, 2, lambda v, m: swap(v, 'dp', dp_ways, m))
    plane = (dp >> 1, dp_ways // 2, lambda v, m: swap(v, 'dp', dp_ways, 2 * m))
    column = (tp, tp_ways, lambda v, m: swap(v, 'tp', tp_ways, m))
    for level in (plane, column):
        x = scatter_sum(x, *level)
    for level in (column, plane, core):
        x = gather(x, *level)
    return x


def solution(mesh):
    tp_ways, dp_ways = mesh.shape['tp'], mesh.shape['dp']

    def local_fit(design_blk, target_blk, ridge):
        rows_dev, _ = design_blk.shape
        sub_rows = rows_dev // tp_ways
        width = NB // tp_ways
        tp = lax.axis_index('tp')
        target_part = lax.dynamic_slice_in_dim(target_blk, tp * sub_rows, sub_rows)
        *panels, last = sweep(design_blk, target_part[:, None], tp_ways, dp_ways)
        last = sum_rest(last, tp_ways, dp_ways)
        moments = [panel[NB - 2:, :NB // 2] for panel in panels] + [last[-2:, :NB // 2]]

        uppers, tops, inverses = [], [], []
        for k in range(PANELS):
            inverses.append(diag_inverse(panels[k], ridge))
            if k < PANELS - 1:
                upper = jnp.dot(inverses[k], panels[k][:, NB:], precision=HIGHEST, preferred_element_type=F32)
                uppers.append(upper)
                for r in range(k + 1, PANELS):
                    right = upper[:, NB * (r - k - 1):]
                    if r == PANELS - 1:
                        right = lax.optimization_barrier(right)
                    panels[r] = panels[r] - gram(right[:, :NB], right)
        corner = last[NB * LAST:]
        rest = last[:NB * LAST]
        for k in range(PANELS):
            tops.append(jnp.dot(inverses[k], rest[:NB], precision=HIGHEST, preferred_element_type=F32))
            if k < PANELS - 1:
                rest = rest[NB:] - gram(uppers[k], tops[k])
            corner = corner - gram(tops[k], tops[k])
        inverses.append(diag_inverse(corner, ridge))
        moment = jnp.concatenate([m.reshape(1, NB) for m in moments], axis=0)
        order, residual = finish(moment, target_blk, design_blk, uppers, tops, inverses, tp_ways)
        coeffs = order.reshape(CHUNKS, tp_ways, width).transpose(1, 0, 2).reshape(-1)
        return coeffs, residual.reshape(-1)

    return jax.shard_map(local_fit, mesh=mesh, in_specs=(P('dp', 'tp'), P('dp'), P()), out_specs=(P(), P('dp')), check_vma=False)
```

```python
import functools

import jax
import jax.numpy as jnp
from jax import lax
from jax.experimental import pallas as pl
from jax.experimental.pallas import tpu as pltpu
from jax.sharding import PartitionSpec as P


LANES = 128
SUB = 8
BLK = 128
NB = 512
CHUNKS = 5
MESH = pl.DeviceIdType.MESH
F32 = jnp.float32
BF16 = jnp.bfloat16


def split3(x):
    hi = x.astype(BF16)
    rest = x - hi.astype(F32)
    mid = rest.astype(BF16)
    low = (rest - mid.astype(F32)).astype(BF16)
    return hi, mid, low


def lhs_cat(x):
    hi, mid, low = split3(x)
    return jnp.concatenate([hi, mid, hi, low, mid, hi], axis=1)


def rhs_cat(x):
    hi, mid, low = split3(x)
    return jnp.concatenate([mid, hi, low, hi, mid, hi], axis=0)


def dot_cat(lhs, rhs):
    return lax.dot_general(lhs, rhs, (((1,), (0,)), ((), ())), preferred_element_type=F32)


def row_sums(parts, sub):
    for shift in (4, 2, 1):
        low = (sub & shift) == 0
        nxt = []
        for t in range(shift):
            a, b = parts[t], parts[t + shift]
            keep = jnp.where(low, a, b)
            move = jnp.where(low, b, a)
            nxt.append(keep + xor_roll(move, shift, sub))
        parts = nxt
    return parts[0]


def xor_roll(x, shift, sub):
    if shift == 4:
        return pltpu.roll(x, 4, 0)
    low = (sub & shift) == 0
    return jnp.where(low, pltpu.roll(x, SUB - shift, 0), pltpu.roll(x, shift, 0))


def bcast_lane(x, c):
    return jnp.broadcast_to(x[:, c:c + 1], (SUB, LANES))


def bcast_row(x, p):
    return jnp.broadcast_to(x[p:p + 1, :], (SUB, LANES))


def factor_block(load, sub, lane):
    octs = BLK // SUB
    a = [load(o) for o in range(octs)]
    e = [jnp.where(lane == sub + SUB * o, 1.0, 0.0).astype(F32) for o in range(octs)]
    out = [None] * octs
    for t in range(octs // 2):
        o0, o1 = 2 * t, 2 * t + 1
        c0 = 16 * t
        r0, r1, e0, e1 = a[o0], a[o1], e[o0], e[o1]
        b0 = [bcast_lane(r0, c0 + q) for q in range(16)]
        b1 = [bcast_lane(r1, c0 + q) for q in range(16)]
        d0 = jnp.ones((SUB, LANES), F32)
        d1 = jnp.ones((SUB, LANES), F32)
        w0 = jnp.ones((SUB, LANES), F32)
        w1 = jnp.ones((SUB, LANES), F32)
        for p in range(16):
            ps = p % 8
            first = p < 8
            piv = bcast_row(b0[p] if first else b1[p], ps)
            inv = 1.0 / piv
            if first:
                d0 = jnp.where(sub == ps, piv, d0)
                w0 = jnp.where(sub == ps, inv, w0)
                m0 = jnp.where(sub > ps, b0[p] * inv, 0.0)
                m1 = b1[p] * inv
            else:
                d1 = jnp.where(sub == ps, piv, d1)
                w1 = jnp.where(sub == ps, inv, w1)
                m1 = jnp.where(sub > ps, b1[p] * inv, 0.0)
            for q in range(p + 1, 16):
                row = bcast_row(b0[q] if first else b1[q], ps)
                if first and ps < 7:
                    b0[q] = b0[q] - m0 * row
                b1[q] = b1[q] - m1 * row
            rr, re = bcast_row(r0 if first else r1, ps), bcast_row(e0 if first else e1, ps)
            if first and ps < 7:
                r0 = r0 - m0 * rr
                e0 = e0 - m0 * re
            r1 = r1 - m1 * rr
            e1 = e1 - m1 * re
        out[o0], out[o1] = e0 * lax.rsqrt(d0), e1 * lax.rsqrt(d1)
        u0, u1, v0, v1 = r0 * w0, r1 * w1, e0 * w0, e1 * w1
        for o in range(2 * t + 2, octs):
            xs, ys = [], []
            for k in range(SUB):
                i = SUB * o + k
                g0, g1 = bcast_lane(r0, i), bcast_lane(r1, i)
                xs.append(g0 * u0 + g1 * u1)
                ys.append(g0 * v0 + g1 * v1)
            a[o] = a[o] - row_sums(xs, sub)
            e[o] = e[o] - row_sums(ys, sub)
    return out


def open_block(work, block, lam):
    n = work.shape[0]
    row = lax.broadcasted_iota(jnp.int32, (n, n), 0)
    col = lax.broadcasted_iota(jnp.int32, (n, n), 1)
    work[:, :n] = block + jnp.where(row == col, lam, 0.0)
    work[:, n:] = jnp.where(row == col, 1.0, 0.0)


def eliminate(work, k):
    n = work.shape[0]
    steps = n // BLK
    sub = lax.broadcasted_iota(jnp.int32, (SUB, LANES), 0)
    lane = lax.broadcasted_iota(jnp.int32, (SUB, LANES), 1)
    base = pl.multiple_of(k * BLK, BLK)
    win = pl.ds(pl.multiple_of(base + BLK, BLK), n)
    diag = pl.ds(base, BLK)

    def load(o):
        return work[pl.ds(pl.multiple_of(base + SUB * o, SUB), SUB), diag]

    inv = jnp.concatenate(factor_block(load, sub, lane), axis=0)
    panel = dot_cat(lhs_cat(inv), rhs_cat(work[diag, win]))
    work[diag, win] = panel
    right = rhs_cat(panel)
    for j in range(steps - 1):
        @pl.when(k == j)
        def _(j=j):
            rows = n - BLK * (j + 1)
            left = lhs_cat(panel[:, :rows].T)
            w = (pl.ds(BLK * (j + 1), rows), pl.ds(BLK * (j + 1), n))
            work[w] = work[w] - dot_cat(left, right)


def invert(work, block, lam):
    open_block(work, block, lam)

    def step(k, carry):
        eliminate(work, k)
        return carry

    lax.fori_loop(0, work.shape[0] // BLK, step, 0)


def diag_kernel(lam_ref, s_ref, w_ref, work):
    invert(work, s_ref[...], lam_ref[0])
    w_ref[...] = work[:, s_ref.shape[0]:]


def diag_inverse(panel, lam):
    n = panel.shape[0]
    return pl.pallas_call(
        diag_kernel,
        out_shape=jax.ShapeDtypeStruct((n, n), F32),
        grid=(1,),
        in_specs=[pl.BlockSpec(memory_space=pltpu.SMEM), pl.BlockSpec((n, n), lambda i: (0, 0))],
        out_specs=pl.BlockSpec((n, n), lambda i: (0, 0)),
        scratch_shapes=[pltpu.VMEM((n, 2 * n), F32)],
        cost_estimate=pl.CostEstimate(flops=20_000_000_000, bytes_accessed=8 * n * n, transcendentals=0),
        name="diag_inverse",
    )(lam.reshape(1), panel)


def close_kernel(ways, lam_ref, h_ref, s_ref, a_hbm, *refs):
    n, pairs = CHUNKS, [(j, c) for c in range(CHUNKS) for j in range(c)]
    panels, tops, inverses, refs = refs[:LAST - 1], refs[LAST - 1:2 * LAST - 1], refs[2 * LAST - 1:3 * LAST - 1], refs[3 * LAST - 1:]
    x_ref, fit_ref, near, a_ref, work, load_sem, a_sem = refs
    hbm = [tops[j] if c == LAST else panels[j].at[:, pl.ds(NB * (c - j - 1), NB)] for j, c in pairs] + list(inverses)
    rows_dev = a_ref.shape[0]
    quarter = rows_dev // a_sem.shape[0]
    spans = [pl.ds(quarter * i, quarter) for i in range(a_sem.shape[0])]
    copies = [pltpu.make_async_copy(ref, near.at[i], load_sem.at[i]) for i, ref in enumerate(hbm)]
    copies += [pltpu.make_async_copy(a_hbm.at[span], a_ref.at[span], a_sem.at[i]) for i, span in enumerate(spans)]
    for copy in copies:
        copy.start()
    invert(work, s_ref[...], lam_ref[0])
    for copy in copies:
        copy.wait()

    def upper(j, c):
        return near[pairs.index((j, c))]

    def inverse(c):
        return near[len(pairs) + c] if c < LAST else work[:, NB:]

    half = []
    for c in range(n):
        right = h_ref[c:c + 1, :]
        for j in range(c):
            right = right - jnp.sum(upper(j, c) * half[j], axis=0, keepdims=True)
        half.append(jnp.sum(inverse(c) * right, axis=1, keepdims=True))
    for c in reversed(range(n)):
        left = half[c]
        for k in range(c + 1, n):
            left = left - jnp.sum(upper(c, k) * x_ref[k:k + 1, :], axis=1, keepdims=True)
        x_ref[c:c + 1, :] = jnp.sum(inverse(c) * left, axis=0, keepdims=True)

    width = NB // ways
    lanes = pl.ds(pl.multiple_of(lax.axis_index("tp") * width, LANES), width)
    mine = [x_ref[c:c + 1, lanes] for c in range(n)]
    group = 4 if rows_dev % (4 * BLK) == 0 else 1

    def product(i, carry):
        for k in range(group):
            at = i * group + k
            rows = pl.ds(pl.multiple_of(at * BLK, BLK), BLK)
            terms = [a_ref[rows, width * c:width * (c + 1)] * mine[c] for c in range(n)]
            total = terms[0]
            for term in terms[1:]:
                total = total + term
            fit_ref[pl.ds(at, 1), :] = jnp.sum(total.T, axis=0, keepdims=True)
        return carry

    lax.fori_loop(0, rows_dev // (group * BLK), product, 0)


def close(ridge, moment, corner, design_blk, uppers, tops, inverses, ways):
    blocks = CHUNKS * (CHUNKS + 1) // 2 - 1
    parts = [*uppers, *tops, *inverses]
    rows_dev, cols_dev = design_blk.shape
    smem, vmem, hbm = (pl.BlockSpec(memory_space=space) for space in (pltpu.SMEM, pltpu.VMEM, pl.ANY))
    return pl.pallas_call(
        functools.partial(close_kernel, ways),
        out_shape=(jax.ShapeDtypeStruct((CHUNKS, NB), F32), jax.ShapeDtypeStruct((rows_dev // LANES, LANES), F32)),
        in_specs=[smem, vmem, vmem, hbm] + [hbm] * len(parts),
        out_specs=(vmem, vmem),
        scratch_shapes=[
            pltpu.VMEM((blocks, NB, NB), F32),
            pltpu.VMEM((rows_dev, cols_dev), F32),
            pltpu.VMEM((NB, 2 * NB), F32),
            pltpu.SemaphoreType.DMA((blocks,)),
            pltpu.SemaphoreType.DMA((4,)),
        ],
        compiler_params=pltpu.CompilerParams(vmem_limit_bytes=52 * 1024 * 1024),
        cost_estimate=pl.CostEstimate(flops=25_000_000_000, bytes_accessed=32_000_000, transcendentals=0),
        name="close",
    )(ridge.reshape(1), moment, corner, design_blk, *parts)


def share_kernel(ways, part_ref, b_ref, r_ref, fit, send_sem, recv_sem):
    z = lax.axis_index("tp")
    barrier = pltpu.get_barrier_semaphore()
    for m in range(1, ways):
        pl.semaphore_signal(barrier, inc=1, device_id={"tp": z ^ m}, device_id_type=MESH)
    pl.semaphore_wait(barrier, ways - 1)
    copies = [
        pltpu.make_async_remote_copy(
            src_ref=part_ref, dst_ref=fit.at[z], send_sem=send_sem.at[m - 1], recv_sem=recv_sem.at[m - 1],
            device_id={"tp": z ^ m}, device_id_type=MESH)
        for m in range(1, ways)
    ]
    for copy in copies:
        copy.start()
    fit[z] = part_ref[...]
    for copy in copies:
        copy.wait()
    total = fit[0]
    for t in range(1, ways):
        total = total + fit[t]
    r_ref[...] = b_ref[...] - total


def share(part, target_blk, ways):
    vmem = pl.BlockSpec(memory_space=pltpu.VMEM)
    return pl.pallas_call(
        functools.partial(share_kernel, ways),
        out_shape=jax.ShapeDtypeStruct(part.shape, F32),
        in_specs=[vmem, vmem],
        out_specs=vmem,
        scratch_shapes=[
            pltpu.VMEM((ways, *part.shape), F32),
            pltpu.SemaphoreType.DMA((ways - 1,)),
            pltpu.SemaphoreType.DMA((ways - 1,)),
        ],
        compiler_params=pltpu.CompilerParams(collective_id=1, has_side_effects=True),
        name="share",
    )(part, target_blk.reshape(part.shape))


HIGHEST = lax.Precision.HIGHEST
CONTRACT_ROWS = (((0,), (0,)), ((), ()))


def gram(left, right):
    return lax.dot_general(left, right, CONTRACT_ROWS, precision=HIGHEST, preferred_element_type=F32)


PIECES = 6
AHEAD = 2
LAST = CHUNKS - 1
PANELS = LAST
SUMMED = ((0, 3), (3, 3), (6, 4), (10, 5))
WHEN = (
    (11, 12, 14, 15, 16, 17, 18, 20, 21),
    (17, 18, 21, 22, 23, 24, 26, 28, 29),
    (23, 24, 26, 27, 28, 29, 30, 31, 32),
    (29, 30),
)


def ladder(tp_ways, dp_ways):
    pairs = tuple(("tp", 2, 1 << k) for k in range(tp_ways.bit_length() - 1))
    return (("dp", 2, 1), ("dp", dp_ways // 2, 2), *pairs)


def steps_of(levels, g):
    if g == len(SUMMED) - 1:
        return [(False, 0)]
    depths = range(len(levels))
    return [(False, d) for d in depths] + [(True, d) for d in reversed(depths)]


def place(level):
    axis, ways, dist = level
    return lax.rem(lax.axis_index(axis) // dist, ways)


def member(level, m):
    axis, _, dist = level
    return {axis: lax.axis_index(axis) ^ (m * dist)}


def sweep_kernel(levels, ways, a_ref, b_ref, *refs):
    outs, (p_ref, x_ref, right, moment, *got) = refs[:PANELS + 1], refs[PANELS + 1:]
    swap_send, swap_recv, own_sem, send_sem, recv_sem, free_sem, out_sem = got[len(SUMMED):]
    sub_rows = a_ref.shape[0] // ways
    width = a_ref.shape[1] // CHUNKS
    piece = sub_rows // PIECES
    steps = CHUNKS * PIECES
    z = lax.axis_index("tp")
    column = ("tp", ways, 1)

    barrier = pltpu.get_barrier_semaphore()
    count = 0
    for level in (*levels[:2], column):
        for m in range(1, level[1]):
            pl.semaphore_signal(barrier, inc=1, device_id=member(level, m), device_id_type=MESH)
            count += 1
    pl.semaphore_wait(barrier, count)

    def own(c):
        return pltpu.make_async_copy(
            a_ref.at[pl.ds(z * sub_rows, sub_rows), pl.ds(width * c, width)], x_ref.at[c, z], own_sem.at[c])

    def travel(p, m):
        c, r = p // PIECES, lax.rem(p, PIECES)
        rows = pl.ds(pl.multiple_of((z ^ m) * sub_rows + r * piece, SUB), piece)
        cols = pl.ds(pl.multiple_of(c * width, LANES), width)
        return pltpu.make_async_remote_copy(
            src_ref=a_ref.at[rows, cols],
            dst_ref=x_ref.at[c, z, pl.ds(pl.multiple_of(r * piece, SUB), piece)],
            send_sem=swap_send.at[p, m - 1],
            recv_sem=swap_recv.at[p, m - 1],
            device_id=member(column, m),
            device_id_type=MESH,
        )

    def load(c, r):
        rows = pl.ds(pl.multiple_of(r * piece, SUB), piece)
        return jnp.concatenate([x_ref[c, t, rows, :] for t in range(ways)], axis=1)

    def span(g, depth):
        first, n = SUMMED[g]
        start, rows = first * NB, n * NB
        for level in levels[:depth]:
            rows //= level[1]
            start = start + place(level) * rows
        return start, rows

    def part(g, depth, m):
        start, _ = span(g, depth)
        rows = span(g, depth + 1)[1]
        return pl.ds(pl.multiple_of(start + (place(levels[depth]) ^ m) * rows, SUB), rows)

    base = [sum(level[1] - 1 for level in levels[:d]) for d in range(len(levels))]

    def scatter(g, depth, m):
        i = base[depth] + m - 1
        return pltpu.make_async_remote_copy(
            src_ref=p_ref.at[part(g, depth, m)],
            dst_ref=slot(g, depth, m),
            send_sem=send_sem.at[g, 0, i],
            recv_sem=recv_sem.at[g, 0, i],
            device_id=member(levels[depth], m),
            device_id_type=MESH,
        )

    def slot(g, depth, m):
        n = SUMMED[g][1] * NB
        at, rows = 0, n
        for d, level in enumerate(levels[:depth + 1]):
            rows //= level[1]
            if d < depth:
                at += rows * (level[1] - 1)
        return got[g].at[pl.ds(at + rows * (m - 1), rows)]

    def gather(g, depth, m):
        i = base[depth] + m - 1
        return pltpu.make_async_remote_copy(
            src_ref=p_ref.at[part(g, depth, 0)],
            dst_ref=p_ref.at[part(g, depth, 0)],
            send_sem=send_sem.at[g, 1, i],
            recv_sem=recv_sem.at[g, 1, i],
            device_id=member(levels[depth], m),
            device_id_type=MESH,
        )

    def start(back, g, depth):
        if back:
            pl.semaphore_wait(free_sem.at[g, depth], levels[depth][1] - 1)
        for m in range(1, levels[depth][1]):
            (gather if back else scatter)(g, depth, m).start()

    def finish(back, g, depth):
        others = range(1, levels[depth][1])
        for m in others:
            (gather if back else scatter)(g, depth, m).wait()
        if back:
            return
        if (True, depth) in steps_of(levels, g):
            for m in others:
                pl.semaphore_signal(free_sem.at[g, depth], inc=1, device_id=member(levels[depth], m), device_id_type=MESH)
        rows = part(g, depth, 0)
        total = p_ref[rows]
        for m in others:
            total = total + slot(g, depth, m)[...]
        p_ref[rows] = total

    def leave(i):
        c = max(c for c in range(CHUNKS) if c * (c + 1) // 2 <= i)
        k = i - c * (c + 1) // 2
        return pltpu.make_async_copy(
            p_ref.at[pl.ds(NB * i, NB)], outs[k].at[:, pl.ds(NB * (c - k), NB)], out_sem.at[i])

    def leave_last():
        return pltpu.make_async_copy(p_ref.at[part(len(SUMMED) - 1, 0, 0)], outs[PANELS], out_sem.at[SUMMED[-1][0]])

    def stage(g, s):
        order = steps_of(levels, g)
        if s > 0:
            finish(*order[s - 1][:1], g, order[s - 1][1])
        if s < len(order):
            start(order[s][0], g, order[s][1])
        elif g == len(SUMMED) - 1:
            leave_last().start()
        else:
            first, n = SUMMED[g]
            for i in range(first, first + n):
                leave(i).start()

    def stages(p, first):
        for g, when in enumerate(WHEN):
            for s, w in enumerate(when):
                if w < steps and (s == 0) == first:
                    @pl.when(p == w)
                    def _(g=g, s=s):
                        stage(g, s)

    for c in range(CHUNKS):
        own(c).start()
    for p in range(AHEAD):
        for m in range(1, ways):
            travel(p, m).start()

    def step(p, carry):
        c, r = p // PIECES, lax.rem(p, PIECES)
        for m in range(1, ways):
            travel(p, m).wait()

        stages(p, False)

        @pl.when(p + AHEAD < steps)
        def _():
            for m in range(1, ways):
                travel(p + AHEAD, m).start()

        @pl.when(r == 0)
        def _():
            own(c).wait()
            moment[...] = jnp.zeros_like(moment)

        new = load(c, r)
        for i, x in enumerate(split3(new)):
            right[i] = x
        weight = b_ref[pl.ds(pl.multiple_of(r * piece, SUB), piece), :]
        moment[...] += jnp.sum(new * weight, axis=0, keepdims=True)
        corner = lax.div(c * (c + 1), 2)

        def product(j, inner):
            left = split3(load(j, r).T)
            total = None
            for a, b in ((0, 2), (2, 0), (1, 1), (0, 1), (1, 0), (0, 0)):
                term = dot_cat(left[a], right[b])
                total = term if total is None else total + term
            rows = pl.ds(pl.multiple_of((corner + j) * NB, NB), NB)

            @pl.when(r == 0)
            def _():
                p_ref[rows] = total

            @pl.when(r > 0)
            def _():
                p_ref[rows] = p_ref[rows] + total

            return inner

        lax.fori_loop(0, c + 1, product, 0)

        @pl.when(r == PIECES - 1)
        def _():
            last = (corner + c + 1) * NB - SUB
            rows = pl.ds(pl.multiple_of(last, SUB), SUB)
            half = NB // 2
            tail = p_ref[rows, :half]
            row = lax.broadcasted_iota(jnp.int32, tail.shape, 0)
            tail = jnp.where(row == SUB - 2, moment[:, :half], tail)
            p_ref[rows, :half] = jnp.where(row == SUB - 1, moment[:, half:], tail)

        stages(p, True)
        return carry

    lax.fori_loop(0, steps, step, 0)
    for p in range(steps, max(w for when in WHEN for w in when) + 1):
        for g, when in enumerate(WHEN):
            for s, w in enumerate(when):
                if w == p:
                    stage(g, s)
    for i in range(SUMMED[-1][0]):
        leave(i).wait()
    leave_last().wait()


def sweep(design_blk, target_col, tp_ways, dp_ways):
    levels = ladder(tp_ways, dp_ways)
    sub_rows = design_blk.shape[0] // tp_ways
    piece = sub_rows // PIECES
    blocks = CHUNKS * (CHUNKS + 1) // 2
    steps = CHUNKS * PIECES
    peers = sum(level[1] - 1 for level in levels)

    def landing(g):
        rows, total = SUMMED[g][1] * NB, 0
        for back, depth in steps_of(levels, g):
            if not back:
                rows //= levels[depth][1]
                total += rows * (levels[depth][1] - 1)
        return pltpu.VMEM((total, NB), F32)

    return pl.pallas_call(
        functools.partial(sweep_kernel, levels, tp_ways),
        out_shape=[jax.ShapeDtypeStruct((NB, NB * (LAST - k)), F32) for k in range(PANELS)]
        + [jax.ShapeDtypeStruct((CHUNKS * NB // 2, NB), F32)],
        in_specs=[pl.BlockSpec(memory_space=pl.ANY), pl.BlockSpec(memory_space=pltpu.VMEM)],
        out_specs=[pl.BlockSpec(memory_space=pl.ANY)] * (PANELS + 1),
        scratch_shapes=[
            pltpu.VMEM((blocks * NB, NB), F32),
            pltpu.VMEM((CHUNKS, tp_ways, sub_rows, NB // tp_ways), F32),
            pltpu.VMEM((3, piece, NB), BF16),
            pltpu.VMEM((1, NB), F32),
            *(landing(g) for g in range(len(SUMMED))),
            pltpu.SemaphoreType.DMA((steps, tp_ways - 1)),
            pltpu.SemaphoreType.DMA((steps, tp_ways - 1)),
            pltpu.SemaphoreType.DMA((CHUNKS,)),
            pltpu.SemaphoreType.DMA((len(SUMMED), 2, peers)),
            pltpu.SemaphoreType.DMA((len(SUMMED), 2, peers)),
            pltpu.SemaphoreType.REGULAR((len(SUMMED), len(levels))),
            pltpu.SemaphoreType.DMA((SUMMED[-1][0] + 1,)),
        ],
        compiler_params=pltpu.CompilerParams(collective_id=0, has_side_effects=True, vmem_limit_bytes=60 * 1024 * 1024),
        cost_estimate=pl.CostEstimate(flops=300_000_000_000, bytes_accessed=32_000_000, transcendentals=0),
        name="sweep",
    )(design_blk, target_col)


def swap(x, axis, ways, mask):
    return lax.ppermute(x, axis, [(i, i ^ mask) for i in range(ways)])


def pick(stack, i):
    return lax.dynamic_index_in_dim(stack, i, 0, keepdims=False)


def scatter_sum(x, me, ways, send):
    parts = x.reshape(ways, -1, x.shape[1])
    total = pick(parts, me)
    for m in range(1, ways):
        total = total + send(pick(parts, me ^ m), m)
    return total


def gather(x, me, ways, send):
    got = [x] + [send(x, m) for m in range(1, ways)]
    rows = []
    for i in range(ways):
        part = got[ways - 1]
        for m in range(ways - 1):
            part = jnp.where(me == i ^ m, got[m], part)
        rows.append(part)
    return jnp.concatenate(rows, axis=0)


def sum_rest(x, tp_ways, dp_ways):
    tp, dp = lax.axis_index('tp'), lax.axis_index('dp')
    core = (dp & 1, 2, lambda v, m: swap(v, 'dp', dp_ways, m))
    plane = (dp >> 1, dp_ways // 2, lambda v, m: swap(v, 'dp', dp_ways, 2 * m))
    column = (tp, tp_ways, lambda v, m: swap(v, 'tp', tp_ways, m))
    for level in (plane, column):
        x = scatter_sum(x, *level)
    for level in (column, plane, core):
        x = gather(x, *level)
    return x


def solution(mesh):
    tp_ways, dp_ways = mesh.shape['tp'], mesh.shape['dp']

    def local_fit(design_blk, target_blk, ridge):
        rows_dev, _ = design_blk.shape
        sub_rows = rows_dev // tp_ways
        width = NB // tp_ways
        tp = lax.axis_index('tp')
        target_part = lax.dynamic_slice_in_dim(target_blk, tp * sub_rows, sub_rows)
        *panels, last = sweep(design_blk, target_part[:, None], tp_ways, dp_ways)
        last = sum_rest(last, tp_ways, dp_ways)
        moments = [panel[NB - 2:, :NB // 2] for panel in panels] + [last[-2:, :NB // 2]]

        uppers, tops, inverses = [], [], []
        for k in range(PANELS):
            inverses.append(diag_inverse(panels[k], ridge))
            if k < PANELS - 1:
                upper = jnp.dot(inverses[k], panels[k][:, NB:], precision=HIGHEST, preferred_element_type=F32)
                uppers.append(upper)
                for r in range(k + 1, PANELS):
                    right = upper[:, NB * (r - k - 1):]
                    if r == PANELS - 1:
                        right = lax.optimization_barrier(right)
                    panels[r] = panels[r] - gram(right[:, :NB], right)
        corner = last[NB * LAST:]
        rest = last[:NB * LAST]
        for k in range(PANELS):
            tops.append(jnp.dot(inverses[k], rest[:NB], precision=HIGHEST, preferred_element_type=F32))
            if k < PANELS - 1:
                rest = rest[NB:] - gram(uppers[k], tops[k])
            corner = corner - gram(tops[k], tops[k])
        moment = jnp.concatenate([m.reshape(1, NB) for m in moments], axis=0)
        order, part = close(ridge, moment, corner, design_blk, uppers, tops, inverses, tp_ways)
        residual = share(part, target_blk, tp_ways)
        coeffs = order.reshape(CHUNKS, tp_ways, width).transpose(1, 0, 2).reshape(-1)
        return coeffs, residual.reshape(-1)

    return jax.shard_map(local_fit, mesh=mesh, in_specs=(P('dp', 'tp'), P('dp'), P()), out_specs=(P(), P('dp')), check_vma=False)
```
